32 devices in a mesh: seq: 8 (over y, x, core), head: 4 (over z).
Axes of the slice: x: 2, y: 2, z: 4, core: 2. Of those that a mesh axis runs over, the one named last changes fastest.
Arguments:
- key_rows: bfloat16 [2048, 2048], P('seq', 'head'), may hold values from -1 to 1, as said below
- values: bfloat16 [2048, 2048], P('seq', 'head'), may hold values from -6 to 6
- d_layer: bfloat16 [2048, 2048], P('seq', 'head'), may hold values from -6 to 6
- out_weight: bfloat16 [2048, 2048], P('head'), may hold values from -0.125 to 0.125
- saved_solutions: float32 [2048, 2048], P('seq', 'head'), may hold values from -0.625 to 0.625
- ridge_scale: float32 [16], P('head'), may hold values from 0.5 to 4
Outputs:
- grad_queries: float32 [2048, 2048], P('seq', 'head')
- grad_keys: float32 [2048, 2048], P('seq', 'head')
- grad_values: float32 [2048, 2048], P('seq', 'head')
The draws below stay inside these ranges and needn't reach their ends.
Inputs may be any that keep to these rules, and one draw needn't show every extreme that they name: `key_rows`: within each head the 128 entries of a key have Euclidean norm 1 up to bfloat16 rounding.
All inputs are finite; a program needn't handle non-finite values.
Results may differ from the reference program's by a relative error of at most 0.0029.
Values may be sent and summed in bfloat16 or wider, within the bound.
A program may use at most 64 MiB of HBM per device.

```python
import math
import jax
import jax.numpy as jnp
from jax import lax

DM = 2048
HEADS = 16
DH = 128
TOK_DEV = 256
ITERS = 8
WIN = 512
TOKENS = 2048


def draw_key_rows(key, part):
    scale_key = jax.random.fold_in(key, 11)
    entry_key = jax.random.fold_in(key, 23)
    channel_scales = jnp.exp(jax.random.uniform(scale_key, (HEADS * DH,), jnp.float32, jnp.log(0.3), jnp.log(1.5)))
    entries = jnp.clip(jax.random.normal(entry_key, (TOKENS, HEADS * DH), jnp.float32), -6.0, 6.0)
    scaled = (entries * channel_scales).reshape(TOKENS, HEADS, DH)
    lengths = jnp.sqrt(jnp.sum(scaled * scaled, axis=-1, keepdims=True) + 1e-06)
    return (scaled / lengths).reshape(TOKENS, HEADS * DH).astype(jnp.bfloat16)


def levels(stream_key, extent, cuts, least, largest):
    level, own = 1.0, jax.random.fold_in(stream_key, 6)
    for axis_at, parts in cuts:
        steps = jnp.exp(jax.random.uniform(jax.random.fold_in(own, axis_at), (parts,), jnp.float32, least / len(cuts), largest / len(cuts)))
        level = level * jnp.repeat(steps, extent[axis_at] // parts).reshape([-1 if axis == axis_at else 1 for axis in range(len(extent))])
    return level


def normal_values(stream_key, extent, spread, bound, pieces=(), kind=jnp.bfloat16):
    factor_of = levels(stream_key, extent, pieces, -0.22, 0.18) if pieces else 1.0
    values = jax.random.normal(stream_key, extent, jnp.float32) * spread * factor_of
    return jnp.minimum(jnp.maximum(values, -bound), bound).astype(kind)


def setup_inputs(seed: int = 0) -> dict:
    arg_keys = jax.random.split(jax.random.key(seed), 7)
    key_rows = draw_key_rows(jax.random.fold_in(arg_keys[6], 71), 0)
    values = normal_values(arg_keys[1], (TOKENS, HEADS * DH), 1.0, 6.0, ((0, 8), (1, 4)))
    d_layer = normal_values(arg_keys[2], (TOKENS, DM), 1.0, 6.0, ((0, 8), (1, 4)))
    out_weight = normal_values(arg_keys[3], (HEADS * DH, DM), DM ** -0.5, 0.125, ((0, 4),))
    saved_solutions = normal_values(arg_keys[4], (TOKENS, HEADS * DH), (WIN ** -0.5), 0.625, ((0, 8), (1, 4)), jnp.float32)
    ridge_scale = jnp.clip(jnp.exp(math.log(4.0) - 2.0794415 * jax.random.uniform(arg_keys[5], (HEADS,), jnp.float32) ** levels(arg_keys[5], (HEADS,), ((0, 4),), -0.2, 0.2)), 0.5, 4.0)
    return dict(key_rows=key_rows, values=values, d_layer=d_layer, out_weight=out_weight, saved_solutions=saved_solutions, ridge_scale=ridge_scale)


HIGHEST_PRECISION = lax.Precision.HIGHEST
EPSILON = 1e-6


def make_lower(block_len):
    row_ids = lax.broadcasted_iota(jnp.int32, (block_len, block_len), 0)
    col_ids = lax.broadcasted_iota(jnp.int32, (block_len, block_len), 1)
    return (row_ids >= col_ids).astype(jnp.float32)


def shift_down(blocks, amount):
    padding = jnp.zeros((amount,) + blocks.shape[1:], blocks.dtype)
    return jnp.concatenate([padding, blocks[: blocks.shape[0] - amount]], axis=0)


def shift_up(blocks, amount):
    padding = jnp.zeros((amount,) + blocks.shape[1:], blocks.dtype)
    return jnp.concatenate([blocks[amount:], padding], axis=0)


def masked_apply(left, right, carried, mask_table):
    scores = jnp.einsum("bid,bjd->bij", left, right, precision=HIGHEST_PRECISION) * mask_table
    return jnp.einsum("bij,bjd->bid", scores, carried, precision=HIGHEST_PRECISION)


def outer_sums(left, right):
    return jnp.einsum("bid,bie->bde", left, right, precision=HIGHEST_PRECISION)


def one_head(operands):
    key_part, value_part, saved_part, dout_part, ridge_value = operands
    block_len = min(512, TOK_DEV)
    block_count = TOKENS // block_len
    lag_blocks = WIN // block_len
    key_blk = key_part.reshape(block_count, block_len, DH)
    val_blk = value_part.reshape(block_count, block_len, DH)
    sav_blk = saved_part.reshape(block_count, block_len, DH)
    out_blk = dout_part.reshape(block_count, block_len, DH)
    lower_table = make_lower(block_len)
    upper_table = lower_table.T

    gram_blocks = outer_sums(key_blk, key_blk)
    state_blocks = outer_sums(val_blk, key_blk)
    gram_before = jnp.cumsum(gram_blocks, axis=0) - gram_blocks
    state_before = jnp.cumsum(state_blocks, axis=0) - state_blocks
    gram_base = gram_before - shift_down(gram_before, lag_blocks)
    state_base = state_before - shift_down(state_before, lag_blocks)
    key_lag = shift_down(key_blk, lag_blocks)
    val_lag = shift_down(val_blk, lag_blocks)

    adjoint_rhs = jnp.einsum("bif,bfe->bie", out_blk, state_base, precision=HIGHEST_PRECISION)
    adjoint_rhs = adjoint_rhs + masked_apply(out_blk, val_blk, key_blk, lower_table)
    adjoint_rhs = adjoint_rhs - masked_apply(out_blk, val_lag, key_lag, lower_table)

    def apply_gram(vectors):
        result = jnp.einsum("bid,bde->bie", vectors, gram_base, precision=HIGHEST_PRECISION)
        result = result + masked_apply(vectors, key_blk, key_blk, lower_table)
        result = result - masked_apply(vectors, key_lag, key_lag, lower_table)
        return result + ridge_value * vectors

    solution = jnp.zeros_like(adjoint_rhs)
    residual_now = adjoint_rhs
    direction = adjoint_rhs
    norm_now = jnp.sum(residual_now * residual_now, axis=-1, keepdims=True)
    for iteration in range(ITERS):
        image = apply_gram(direction)
        alpha = norm_now / (jnp.sum(direction * image, axis=-1, keepdims=True) + EPSILON)
        solution = solution + alpha * direction
        residual_now = residual_now - alpha * image
        norm_next = jnp.sum(residual_now * residual_now, axis=-1, keepdims=True)
        direction = residual_now + (norm_next / (norm_now + EPSILON)) * direction
        norm_now = norm_next

    pair_blocks = outer_sums(solution, sav_blk)
    cross_blocks = outer_sums(sav_blk, out_blk)
    pair_after = jnp.flip(jnp.cumsum(jnp.flip(pair_blocks, 0), axis=0), 0) - pair_blocks
    cross_after = jnp.flip(jnp.cumsum(jnp.flip(cross_blocks, 0), axis=0), 0) - cross_blocks
    pair_base = pair_after - shift_up(pair_after, lag_blocks)
    cross_base = cross_after - shift_up(cross_after, lag_blocks)
    sym_base = pair_base + jnp.swapaxes(pair_base, 1, 2)

    sol_lead = shift_up(solution, lag_blocks)
    sav_lead = shift_up(sav_blk, lag_blocks)
    out_lead = shift_up(out_blk, lag_blocks)

    grad_k = -jnp.einsum("bid,bde->bie", key_blk, sym_base, precision=HIGHEST_PRECISION)
    grad_k = grad_k + jnp.einsum("bif,bef->bie", val_blk, cross_base, precision=HIGHEST_PRECISION)
    grad_k = grad_k - masked_apply(key_blk, sav_blk, solution, upper_table)
    grad_k = grad_k - masked_apply(key_blk, solution, sav_blk, upper_table)
    grad_k = grad_k + masked_apply(val_blk, out_blk, sav_blk, upper_table)
    grad_k = grad_k + masked_apply(key_blk, sav_lead, sol_lead, upper_table)
    grad_k = grad_k + masked_apply(key_blk, sol_lead, sav_lead, upper_table)
    grad_k = grad_k - masked_apply(val_blk, out_lead, sav_lead, upper_table)

    grad_v = jnp.einsum("bid,bdf->bif", key_blk, cross_base, precision=HIGHEST_PRECISION)
    grad_v = grad_v + masked_apply(key_blk, sav_blk, out_blk, upper_table)
    grad_v = grad_v - masked_apply(key_blk, sav_lead, out_lead, upper_table)

    return (solution.reshape(TOKENS, DH), grad_k.reshape(TOKENS, DH), grad_v.reshape(TOKENS, DH))


def reference(key_rows, values, d_layer, out_weight, saved_solutions, ridge_scale):
    d_heads = jnp.dot(d_layer, out_weight.T, preferred_element_type=jnp.float32).astype(jnp.bfloat16)

    def by_head(array):
        return array.astype(jnp.float32).reshape(TOKENS, HEADS, DH).transpose(1, 0, 2)

    grads = lax.map(one_head, (by_head(key_rows), by_head(values), by_head(saved_solutions),
                               by_head(d_heads), ridge_scale.astype(jnp.float32)))

    def by_token(array):
        return array.transpose(1, 0, 2).reshape(TOKENS, HEADS * DH).astype(jnp.float32)

    return by_token(grads[0]), by_token(grads[1]), by_token(grads[2])
```

```python
import functools
import jax
import jax.numpy as jnp
from jax import lax
from jax.experimental import pallas as pl
from jax.experimental.pallas import tpu as pltpu
from jax.sharding import PartitionSpec as P

DH = 128
ITERS = 8
EPSILON = 1e-06
BF = jnp.bfloat16
F32 = jnp.float32
MESH = pl.DeviceIdType.MESH


def nn(left, right):
    return lax.dot_general(left, right, (((1,), (0,)), ((), ())), preferred_element_type=F32)


def nt(left, right):
    return lax.dot_general(left, right, (((1,), (1,)), ((), ())), preferred_element_type=F32)


def split(a):
    hi = a.astype(BF)
    return hi, (a - hi.astype(F32)).astype(BF)


def flip(a):
    return a.astype(F32).T.astype(BF)


def beside(*parts):
    return jnp.concatenate(parts, axis=1)


def above(*parts):
    return jnp.concatenate(parts, axis=0)


def own_mask(tok):
    key_ids = lax.broadcasted_iota(jnp.int32, (tok, tok), 0)
    tok_ids = lax.broadcasted_iota(jnp.int32, (tok, tok), 1)
    return key_ids <= tok_ids


def window_masked(scores):
    tok = scores.shape[1]
    own = own_mask(tok)
    return above(jnp.where(own, scores[:tok], 0.0), jnp.where(own, 0.0, scores[tok:]))


def slots_sum(ref, h):
    total = ref[0, h].astype(F32)
    for slot in range(1, ref.shape[0]):
        total = total + ref[slot, h].astype(F32)
    return total


def mega(span, n_seq, n_head, ridge_hbm, key_hbm, val_hbm, d_hbm, w_hbm, sav_hbm, sol, gk, gv,
         ridge, key, val, d_all, w, sav, out, key_lag, val_lag,
         gram, state, cross, sym, gram_in, state_in, cross_in, sym_in,
         gkl, gvl, gkl_bf, gvl_bf, gkl_in, gvl_in,
         k2_s, kt_s, a1_s, vs_s, xt_s, full_s, g_s, st_s, sym_s, r_s, p_s, y_s, rr_s,
         local_sem, dsend_sem, drecv_sem, send_sem, recv_sem):
    s = lax.axis_index("seq")
    me = lax.axis_index("head")
    heads = ridge.shape[0]
    tok = key.shape[0]
    half = tok // 2
    width = d_all.shape[2]
    mids_exist = span > 1
    rows = [slice(0, half), slice(half, tok)]
    d_copy_in = pltpu.make_async_copy(d_hbm, d_all.at[me], local_sem.at[0])
    key_copy = pltpu.make_async_copy(key_hbm, key, local_sem.at[1])
    val_copy = pltpu.make_async_copy(val_hbm, val, local_sem.at[2])
    w_copy = pltpu.make_async_copy(w_hbm, w, local_sem.at[3])
    x_copy = pltpu.make_async_copy(sav_hbm, sav, local_sem.at[4])
    ridge_copy = pltpu.make_async_copy(ridge_hbm, ridge, local_sem.at[5])
    for copy in (d_copy_in, key_copy, val_copy, x_copy, w_copy, ridge_copy):
        copy.start()

    def exists(d):
        return s + d < n_seq if d > 0 else s + d >= 0

    barrier = pltpu.get_barrier_semaphore()
    has_right, has_left = me + 1 < n_head, me > 0
    for there, step in ((has_right, 1), (has_left, -1)):
        @pl.when(there)
        def _():
            pl.semaphore_signal(barrier, inc=1, device_id={"head": me + step}, device_id_type=MESH)
    for d in [d for m in range(1, span + 1) for d in (m, -m)]:
        @pl.when(exists(d))
        def _():
            pl.semaphore_signal(barrier, inc=1, device_id={"seq": s + d}, device_id_type=MESH)
    pl.semaphore_wait(
        barrier,
        jnp.minimum(me, 1) + jnp.minimum(n_head - 1 - me, 1)
        + jnp.minimum(s, span) + jnp.minimum(n_seq - 1 - s, span),
    )

    counter = [0]
    sends = []

    class Hop:
        def __init__(self, source, target, d):
            self.d = d
            self.copy = pltpu.make_async_remote_copy(
                src_ref=source,
                dst_ref=target,
                send_sem=send_sem.at[counter[0]],
                recv_sem=recv_sem.at[counter[0]],
                device_id={"seq": s + d},
                device_id_type=MESH,
            )
            counter[0] += 1
            sends.append(self)

            @pl.when(jnp.logical_not(exists(-d)))
            def _():
                target[...] = jnp.zeros(target.shape, target.dtype)

        def start(self):
            pl.when(exists(self.d))(self.copy.start)
            return self

        def arrive(self):
            pl.when(exists(-self.d))(self.copy.wait_recv)

        def finish(self):
            pl.when(exists(self.d))(self.copy.wait_send)

    def mids(source, target, sign):
        return [Hop(source, target.at[m - 1], sign * m).start() for m in range(1, span)]

    def d_copy(origin, c, step):
        piece = d_all.at[origin, pl.ds(c * half, half)]
        place = origin * 2 + c
        return pltpu.make_async_remote_copy(
            src_ref=piece,
            dst_ref=piece,
            send_sem=dsend_sem.at[place + (0 if step > 0 else 2 * n_head)],
            recv_sem=drecv_sem.at[place],
            device_id={"head": me + step},
            device_id_type=MESH,
        )

    def d_start(c):
        pl.when(has_right)(lambda: d_copy(me, c, 1).start())
        pl.when(has_left)(lambda: d_copy(me, c, -1).start())

    def d_relay(c):
        for k in range(1, n_head - 1):
            @pl.when(jnp.logical_and(me - k >= 0, has_right))
            def _():
                copy = d_copy(me - k, c, 1)
                copy.wait_recv()
                copy.start()

            @pl.when(jnp.logical_and(me + k < n_head, has_left))
            def _():
                copy = d_copy(me + k, c, -1)
                copy.wait_recv()
                copy.start()

    at_end = jnp.logical_or(me == 0, me == n_head - 1)

    def project(c):
        acc = None
        for i in range(n_head):
            origin = jnp.where(me == 0, i, n_head - 1 - i)
            if i:
                pl.when(at_end)(lambda: d_copy(origin, c, 1).wait_recv())
            col = pl.multiple_of(origin * width, width)
            part = nt(d_all[origin, rows[c]], w[:, pl.ds(col, width)])
            acc = part if acc is None else acc + part
        out[rows[c]] = acc.astype(BF)

    def cols(h):
        return slice(h * DH, (h + 1) * DH)

    d_copy_in.wait()
    d_start(0)
    key_copy.wait()
    key_hop = Hop(key, key_lag, span).start()
    val_copy.wait()
    val_hop = Hop(val, val_lag, span).start()
    for h in range(heads):
        total = None
        for c in range(2):
            k = key[rows[c], cols(h)]
            kt = flip(k)
            kt_s[c, h, :, :half] = kt
            k2_s[c, h, :half] = beside(k, k)
            both = nn(kt, beside(k, val[rows[c], cols(h)]))
            if c == 0:
                full_s[1, h] = both
            total = both if total is None else total + both
        gram[h] = total[:, :DH].astype(BF)
        state[h] = total[:, DH:].astype(BF)
    state_hops = mids(state, state_in, 1)
    gram_hops = mids(gram, gram_in, 1)
    d_relay(0)
    d_start(1)
    x_copy.wait()
    for h in range(heads):
        for c in range(2):
            x_hi, x_lo = split(sav[rows[c], cols(h)].T)
            xt_s[c, h] = beside(x_hi, x_lo)
    d_relay(1)
    w_copy.wait()
    ridge_copy.wait()
    project(0)

    key_hop.arrive()
    for h in range(heads):
        for c in range(2):
            k = key_lag[rows[c], cols(h)]
            kt_s[c, h, :, half:] = flip(k)
            k2_s[c, h, half:] = beside(k, k)
            x2 = beside(*split(sav[rows[c], cols(h)]))
            a1 = window_masked(nt(k2_s[c, h], x2))
            a1_s[c, h] = beside(*split(a1))
    val_hop.arrive()
    for h in range(heads):
        lag = rows[1]
        full_s[0, h] = nn(kt_s[1, h, :, half:], beside(key_lag[lag, cols(h)], val_lag[lag, cols(h)]))
    for hop in state_hops + gram_hops:
        hop.arrive()
    for h in range(heads):
        for c in range(2):
            g, st = full_s[c, h, :, :DH], full_s[c, h, :, DH:]
            if mids_exist:
                g = g + slots_sum(gram_in, h)
                st = st + slots_sum(state_in, h)
            g_hi, g_lo = split(g)
            g_s[c, h] = beside(g_hi, g_hi, g_lo)
            st_s[c, h] = beside(*split(st))

    def begin(c):
        for h in range(heads):
            o = out[rows[c], cols(h)]
            v = above(val[rows[c], cols(h)], val_lag[rows[c], cols(h)])
            scores = window_masked(nt(v, o))
            vs_s[c, h] = scores
            s_hi, s_lo = split(scores)
            r = nn(kt_s[c, h], s_hi) + nn(kt_s[c, h], s_lo) + nt(st_s[c, h], beside(o, o))
            r_s[h] = r
            p_s[h] = r
            y_s[h] = jnp.zeros_like(r)
            rr_s[h] = jnp.sum(r * r, axis=0, keepdims=True)

    def cross_part(c):
        for h in range(heads):
            o = out[rows[c], cols(h)]
            o2 = above(o, o)
            both = nn(a1_s[c, h], o2)
            cross_c = nn(xt_s[c, h], o2)
            c_hi, c_lo = split(cross_c)
            if c == 0:
                gv[rows[0], cols(h)] = both[:half]
                gvl[rows[0], cols(h)] = both[half:]
                sym_s[h] = cross_c
                k2, v = k2_s[1, h, half:], val_lag[rows[1], cols(h)]
                gvl[rows[1], cols(h)] = nn(k2, above(c_hi, c_lo))
                gkl[rows[1], cols(h)] = nt(beside(v, v), beside(c_hi, c_lo))
                gvl_bf[rows[0], cols(h)] = both[half:].astype(BF)
            else:
                gv[rows[1], cols(h)] = both[:half]
                gvl_bf[rows[1], cols(h)] = (gvl[rows[1], cols(h)] + both[half:]).astype(BF)
                cross[h] = (sym_s[h] + cross_c).astype(BF)
                k2, v = k2_s[0, h, :half], val[rows[0], cols(h)]
                gv[rows[0], cols(h)] = gv[rows[0], cols(h)] + nn(k2, above(c_hi, c_lo))
                gk[rows[0], cols(h)] = gk[rows[0], cols(h)] + nt(beside(v, v), beside(c_hi, c_lo))

    def solve(c):
        def step(_, carry):
            for h in range(heads):
                p = p_s[h]
                p_hi, p_lo = split(p)
                scores = nn(k2_s[c, h], above(p_hi, p_lo))
                masked = window_masked(scores).astype(BF)
                image = nn(kt_s[c, h], masked) + nn(g_s[c, h], above(p_hi, p_lo, p_hi))
                image = image + ridge[h] * p
                rr = rr_s[h]
                alpha = rr / (jnp.sum(p * image, axis=0, keepdims=True) + EPSILON)
                y_s[h] = y_s[h] + alpha * p
                r = r_s[h] - alpha * image
                r_s[h] = r
                nr = jnp.sum(r * r, axis=0, keepdims=True)
                p_s[h] = r + nr / (rr + EPSILON) * p
                rr_s[h] = nr
            return carry

        lax.fori_loop(0, ITERS, step, 0)

    def key_part(c, h, which):
        y_hi, y_lo = split(y_s[h])
        part = slice(0, half) if which == 0 else slice(half, tok)
        scores = nn(k2_s[c, h, part], above(y_hi, y_lo))
        own = own_mask(half)
        scores = jnp.where(own, scores, 0.0) if which == 0 else jnp.where(own, 0.0, scores)
        a2_hi, a2_lo = split(vs_s[c, h, part] - scores)
        x_hi, x_lo = split(sav[rows[c], cols(h)])
        a1 = a1_s[c, h, part]
        g = nn(beside(a2_hi, a2_lo), above(x_hi, x_hi)) + nn(a2_hi, x_lo)
        return g - nt(a1, beside(y_hi, y_hi)) - nt(a1[:, :half], y_lo)

    def sym_part(c, h):
        y_hi, y_lo = split(-y_s[h])
        pair = nt(xt_s[c, h], beside(y_hi, y_hi)) + nt(xt_s[c, h, :, :half], y_lo)
        return pair + pair.T

    begin(0)
    cross_part(0)
    gva_hop = Hop(gvl_bf.at[pl.ds(0, half)], gvl_in.at[pl.ds(0, half)], -span).start()
    solve(0)
    for h in range(heads):
        gkl_bf[rows[0], cols(h)] = key_part(0, h, 1).astype(BF)
    gka_hop = Hop(gkl_bf.at[pl.ds(0, half)], gkl_in.at[pl.ds(0, half)], -span).start()
    for h in range(heads):
        gk[rows[0], cols(h)] = key_part(0, h, 0)
        sy = sym_part(0, h)
        sym_s[heads + h] = sy
        gkl[rows[1], cols(h)] = gkl[rows[1], cols(h)] + nn(k2_s[1, h, half:], above(*split(sy)))
        sol[rows[0], cols(h)] = y_s[h].T
    project(1)
    begin(1)
    cross_part(1)
    gvb_hop = Hop(gvl_bf.at[pl.ds(half, half)], gvl_in.at[pl.ds(half, half)], -span).start()
    cross_hops = mids(cross, cross_in, -1)
    solve(1)
    for h in range(heads):
        gkl_bf[rows[1], cols(h)] = (gkl[rows[1], cols(h)] + key_part(1, h, 1)).astype(BF)
    gkb_hop = Hop(gkl_bf.at[pl.ds(half, half)], gkl_in.at[pl.ds(half, half)], -span).start()
    for h in range(heads):
        sy = sym_part(1, h)
        sym[h] = (sym_s[heads + h] + sy).astype(BF)
        sym_s[h] = sy
    sym_hops = mids(sym, sym_in, -1)
    for h in range(heads):
        gk[rows[1], cols(h)] = key_part(1, h, 0)
        gk[rows[0], cols(h)] = gk[rows[0], cols(h)] + nn(k2_s[0, h, :half], above(*split(sym_s[h])))
        sol[rows[1], cols(h)] = y_s[h].T
    for hop in [gva_hop, gvb_hop] + cross_hops:
        hop.arrive()
    for h in range(heads):
        v_add = gvl_in[:, cols(h)].astype(F32)
        if mids_exist:
            k, v = key[:, cols(h)], val[:, cols(h)]
            c_hi, c_lo = split(slots_sum(cross_in, h))
            v_add = v_add + nn(beside(k, k), above(c_hi, c_lo))
            gk[:, cols(h)] = gk[:, cols(h)] + nt(beside(v, v), beside(c_hi, c_lo))
        gv[:, cols(h)] = gv[:, cols(h)] + v_add
    for hop in [gka_hop, gkb_hop] + sym_hops:
        hop.arrive()
    for h in range(heads):
        k_add = gkl_in[:, cols(h)].astype(F32)
        if mids_exist:
            k = key[:, cols(h)]
            k_add = k_add + nn(beside(k, k), above(*split(slots_sum(sym_in, h))))
        gk[:, cols(h)] = gk[:, cols(h)] + k_add
    for j in range(n_head):
        for c in range(2):
            pl.when(jnp.logical_and(has_right, j <= me))(lambda: d_copy(j, c, 1).wait_send())
            pl.when(jnp.logical_and(has_left, j >= me))(lambda: d_copy(j, c, -1).wait_send())
    for hop in sends:
        hop.finish()


def store(sol, gk, gv, sol_hbm, gk_hbm, gv_hbm, sem):
    copies = [
        pltpu.make_async_copy(source, target, sem.at[i])
        for i, (source, target) in enumerate([(sol, sol_hbm), (gk, gk_hbm), (gv, gv_hbm)])
    ]
    for copy in copies:
        copy.start()
    for copy in copies:
        copy.wait()


def body(key_rows, values, d_layer, out_weight, saved_solutions, ridge_scale):
    tok, cols = key_rows.shape
    heads = cols // DH
    half = tok // 2
    n_seq, n_head = lax.axis_size("seq"), lax.axis_size("head")
    span = n_seq // 4
    slots = max(span - 1, 1)
    copies = 6 + 4 * (span - 1)
    vmem = pl.BlockSpec(memory_space=pltpu.VMEM)
    hbm = pl.BlockSpec(memory_space=pltpu.HBM)
    flat = jax.ShapeDtypeStruct((tok, cols), F32)
    kept = pltpu.VMEM((tok, cols), F32)
    rows_bf = pltpu.VMEM((tok, cols), BF)
    rows_f = pltpu.VMEM((tok, cols), F32)
    mats = pltpu.VMEM((heads, DH, DH), BF)
    mats_in = pltpu.VMEM((slots, heads, DH, DH), BF)
    vec = pltpu.VMEM((heads, DH, half), F32)
    results = pl.pallas_call(
        functools.partial(mega, span, n_seq, n_head),
        name="layer",
        out_shape=[kept, kept, kept],
        in_specs=[hbm] * 6,
        out_specs=[vmem, vmem, vmem],
        scratch_shapes=[
            pltpu.SMEM((heads,), F32), rows_bf, rows_bf, pltpu.VMEM((n_head,) + d_layer.shape, BF),
            pltpu.VMEM(out_weight.shape, BF), rows_f, rows_bf, rows_bf, rows_bf,
            mats, mats, mats, mats, mats_in, mats_in, mats_in, mats_in,
            rows_f, rows_f, rows_bf, rows_bf, rows_bf, rows_bf,
            pltpu.VMEM((2, heads, tok, 2 * DH), BF),
            pltpu.VMEM((2, heads, DH, tok), BF),
            pltpu.VMEM((2, heads, tok, tok), BF),
            pltpu.VMEM((2, heads, tok, half), F32),
            pltpu.VMEM((2, heads, DH, tok), BF),
            pltpu.VMEM((2, heads, DH, 2 * DH), F32),
            pltpu.VMEM((2, heads, DH, 3 * DH), BF),
            pltpu.VMEM((2, heads, DH, 2 * DH), BF),
            pltpu.VMEM((2 * heads, DH, DH), F32),
            vec, vec, vec,
            pltpu.VMEM((heads, 1, half), F32),
            pltpu.SemaphoreType.DMA((6,)),
            pltpu.SemaphoreType.DMA((4 * n_head,)),
            pltpu.SemaphoreType.DMA((2 * n_head,)),
            pltpu.SemaphoreType.DMA((copies,)),
            pltpu.SemaphoreType.DMA((copies,)),
        ],
        compiler_params=pltpu.CompilerParams(
            collective_id=0, has_side_effects=True, vmem_limit_bytes=48 * 1024 * 1024
        ),
    )(*(
        pltpu.with_memory_space_constraint(array, pltpu.HBM)
        for array in (ridge_scale, key_rows, values, d_layer, out_weight, saved_solutions)
    ))
    return pl.pallas_call(
        store,
        name="store",
        out_shape=[flat, flat, flat],
        in_specs=[vmem, vmem, vmem],
        out_specs=[hbm, hbm, hbm],
        scratch_shapes=[pltpu.SemaphoreType.DMA((3,))],
        compiler_params=pltpu.CompilerParams(vmem_limit_bytes=8 * 1024 * 1024),
    )(*(pltpu.with_memory_space_constraint(result, pltpu.VMEM) for result in results))


def solution(mesh):
    return jax.shard_map(
        body,
        mesh=mesh,
        in_specs=(
            P("seq", "head"),
            P("seq", "head"),
            P("seq", "head"),
            P("head", None),
            P("seq", "head"),
            P("head"),
        ),
        out_specs=(P("seq", "head"), P("seq", "head"), P("seq", "head")),
        check_vma=False,
    )
```

```python
import functools
import jax
import jax.numpy as jnp
from jax import lax
from jax.experimental import pallas as pl
from jax.experimental.pallas import tpu as pltpu
from jax.sharding import PartitionSpec as P

DH = 128
ITERS = 8
EPSILON = 1e-06
BF = jnp.bfloat16
F32 = jnp.float32
MESH = pl.DeviceIdType.MESH


def nn(left, right):
    return lax.dot_general(left, right, (((1,), (0,)), ((), ())), preferred_element_type=F32)


def nt(left, right):
    return lax.dot_general(left, right, (((1,), (1,)), ((), ())), preferred_element_type=F32)


def split(a):
    hi = a.astype(BF)
    return hi, (a - hi.astype(F32)).astype(BF)


def flip(a):
    return a.astype(F32).T.astype(BF)


def beside(*parts):
    return jnp.concatenate(parts, axis=1)


def above(*parts):
    return jnp.concatenate(parts, axis=0)


def own_mask(tok):
    key_ids = lax.broadcasted_iota(jnp.int32, (tok, tok), 0)
    tok_ids = lax.broadcasted_iota(jnp.int32, (tok, tok), 1)
    return key_ids <= tok_ids


def window_masked(scores):
    tok = scores.shape[1]
    own = own_mask(tok)
    return above(jnp.where(own, scores[:tok], 0.0), jnp.where(own, 0.0, scores[tok:]))


def slots_sum(ref, h):
    total = ref[0, h].astype(F32)
    for slot in range(1, ref.shape[0]):
        total = total + ref[slot, h].astype(F32)
    return total


def mega(span, n_seq, n_head, ridge_hbm, key_hbm, val_hbm, d_hbm, w_hbm, sav_hbm, gq, gk, gv,
         ridge, key, val, d_all, w, sav, key_lag, val_lag, o_s,
         mid, mid_lag, mid_in, cross, sym, cross_in, sym_in,
         gkl_bf, gvl_bf, gkl_in, gvl_in, gkl_s, gvl_s, gk_more, gv_more, cross_a, sym_a,
         k2_s, kt_s, vc_s, xs_s, xt_s, a1_s, vs_s, full_s, g_s, st_s, r_s, p_s, ya_s, yb_s, rr_s,
         local_sem, dsend_sem, drecv_sem, send_sem, recv_sem):
    s = lax.axis_index("seq")
    me = lax.axis_index("head")
    heads = ridge.shape[0]
    tok = key.shape[0]
    half = tok // 2
    width = d_all.shape[2]
    rows = [slice(0, half), slice(half, tok)]
    y_s = [ya_s, yb_s]
    d_copy_in = pltpu.make_async_copy(d_hbm, d_all.at[me], local_sem.at[0])
    key_copy = pltpu.make_async_copy(key_hbm, key, local_sem.at[1])
    val_copy = pltpu.make_async_copy(val_hbm, val, local_sem.at[2])
    w_copy = pltpu.make_async_copy(w_hbm, w, local_sem.at[3])
    x_copy = pltpu.make_async_copy(sav_hbm, sav, local_sem.at[4])
    ridge_copy = pltpu.make_async_copy(ridge_hbm, ridge, local_sem.at[5])
    for copy in (d_copy_in, key_copy, val_copy, x_copy, w_copy, ridge_copy):
        copy.start()

    def exists(d):
        return s + d < n_seq if d > 0 else s + d >= 0

    barrier = pltpu.get_barrier_semaphore()
    has_right, has_left = me + 1 < n_head, me > 0
    for there, step in ((has_right, 1), (has_left, -1)):
        @pl.when(there)
        def _():
            pl.semaphore_signal(barrier, inc=1, device_id={"head": me + step}, device_id_type=MESH)
    for d in [d for m in range(1, span + 1) for d in (m, -m)]:
        @pl.when(exists(d))
        def _():
            pl.semaphore_signal(barrier, inc=1, device_id={"seq": s + d}, device_id_type=MESH)
    pl.semaphore_wait(
        barrier,
        jnp.minimum(me, 1) + jnp.minimum(n_head - 1 - me, 1)
        + jnp.minimum(s, span) + jnp.minimum(n_seq - 1 - s, span),
    )

    counter = [0]
    hops = []

    class Hop:
        def __init__(self, source, target, d, sender=None, receiver=None):
            self.sender = exists(d) if sender is None else sender
            self.receiver = exists(-d) if receiver is None else receiver
            self.copy = pltpu.make_async_remote_copy(
                src_ref=source,
                dst_ref=target,
                send_sem=send_sem.at[counter[0]],
                recv_sem=recv_sem.at[counter[0]],
                device_id={"seq": s + d},
                device_id_type=MESH,
            )
            counter[0] += 1
            hops.append(self)
            if receiver is None:
                @pl.when(jnp.logical_not(self.receiver))
                def _():
                    target[...] = jnp.zeros(target.shape, target.dtype)

        def start(self):
            pl.when(self.sender)(self.copy.start)
            return self

        def arrive(self):
            pl.when(self.receiver)(self.copy.wait_recv)

        def finish(self):
            pl.when(self.sender)(self.copy.wait_send)

    def mids(source, target, sign):
        return [Hop(source, target.at[m - 1], sign * m).start() for m in range(1, span)]

    def d_copy(origin, c, step):
        piece = d_all.at[origin, pl.ds(c * half, half)]
        place = origin * 2 + c
        return pltpu.make_async_remote_copy(
            src_ref=piece,
            dst_ref=piece,
            send_sem=dsend_sem.at[place + (0 if step > 0 else 2 * n_head)],
            recv_sem=drecv_sem.at[place],
            device_id={"head": me + step},
            device_id_type=MESH,
        )

    def d_start(c):
        pl.when(has_right)(lambda: d_copy(me, c, 1).start())
        pl.when(has_left)(lambda: d_copy(me, c, -1).start())

    def d_relay(k, c):
        @pl.when(jnp.logical_and(me - k >= 0, has_right))
        def _():
            copy = d_copy(me - k, c, 1)
            copy.wait_recv()
            copy.start()

        @pl.when(jnp.logical_and(me + k < n_head, has_left))
        def _():
            copy = d_copy(me + k, c, -1)
            copy.wait_recv()
            copy.start()

    at_end = jnp.logical_or(me == 0, me == n_head - 1)

    def project(c):
        acc = None
        for i in range(n_head):
            origin = jnp.where(me == 0, i, n_head - 1 - i)
            if i:
                pl.when(at_end)(lambda: d_copy(origin, c, 1).wait_recv())
            col = pl.multiple_of(origin * width, width)
            part = nt(d_all[origin, rows[c]], w[:, pl.ds(col, width)])
            acc = part if acc is None else acc + part
        for h in range(heads):
            o_s[h, rows[c]] = acc[:, h * DH : (h + 1) * DH].astype(BF)

    def cols(h):
        return slice(h * DH, (h + 1) * DH)

    d_copy_in.wait()
    d_start(0)
    d_start(1)
    key_copy.wait()
    key_hop = Hop(key, key_lag, span).start()
    val_copy.wait()
    val_hop = Hop(val, val_lag, span).start()
    for h in range(heads):
        total = None
        for c in range(2):
            k, v = key[rows[c], cols(h)], val[rows[c], cols(h)]
            kt = flip(k)
            kt_s[c, h, :, :half] = kt
            k2_s[c, h, :half] = beside(k, k)
            vc_s[c, h, :half] = v
            both = nn(kt, beside(k, v))
            if c == 0:
                full_s[1, h] = both
            total = both if total is None else total + both
        mid[h] = total.astype(BF)
    paired = span == 2
    if paired:
        odd = lax.rem(s, 2) == 1
        even = jnp.logical_not(odd)
        mid_hops = [Hop(mid, mid_in.at[0], 1, even, odd).start()]
    else:
        mid_hops = mids(mid, mid_in, 1)
    x_copy.wait()
    for h in range(heads):
        xs_s[h] = beside(*split(sav[:, cols(h)]))
        for c in range(2):
            xt_s[c, h] = beside(*split(sav[rows[c], cols(h)].T))
    for k in range(1, n_head - 1):
        for c in range(2):
            d_relay(k, c)
    w_copy.wait()
    ridge_copy.wait()
    key_hop.arrive()
    for h in range(heads):
        for c in range(2):
            k = key_lag[rows[c], cols(h)]
            kt_s[c, h, :, half:] = flip(k)
            k2_s[c, h, half:] = beside(k, k)
    val_hop.arrive()
    for h in range(heads):
        for c in range(2):
            vc_s[c, h, half:] = val_lag[rows[c], cols(h)]
        late = nn(kt_s[1, h, :, half:], beside(k2_s[1, h, half:, :DH], vc_s[1, h, half:]))
        full_s[0, h] = late
        if paired:
            early = nn(kt_s[0, h, :, half:], beside(k2_s[0, h, half:, :DH], vc_s[0, h, half:]))
            mid_lag[h] = (early + late).astype(BF)
    if paired:
        mid_hops.append(Hop(mid_lag, mid_in.at[0], -1, odd, even).start())
    project(0)
    for hop in mid_hops:
        hop.arrive()
    for h in range(heads):
        for c in range(2):
            total = full_s[c, h]
            if span > 1:
                total = total + slots_sum(mid_in, h)
            g_hi, g_lo = split(total[:, :DH])
            g_s[c, h] = beside(g_hi, g_hi)
            st_s[c, h] = beside(*split(total[:, DH:]))

    def begin(c):
        for h in range(heads):
            o = o_s[h, rows[c]]
            scores = window_masked(nt(vc_s[c, h], o))
            vs_s[c, h] = scores
            s_hi, s_lo = split(scores)
            r = nn(kt_s[c, h], s_hi) + nn(kt_s[c, h], s_lo) + nt(st_s[c, h], beside(o, o))
            r_s[h] = r
            p_s[h] = r
            y_s[c][h] = jnp.zeros_like(r)
            rr_s[h] = jnp.sum(r * r, axis=0, keepdims=True)

    def lag_scores(c, h):
        a1_s[c, h] = beside(*split(window_masked(nt(k2_s[c, h], xs_s[h, rows[c]]))))

    def cross_part(c, h):
        o = o_s[h, rows[c]]
        o2 = above(o, o)
        both = nn(a1_s[c, h], o2)
        cross_c = nn(xt_s[c, h], o2)
        c_hi, c_lo = split(cross_c)
        if c == 0:
            k2, v = k2_s[1, h, half:], vc_s[1, h, half:]
            gv[h, rows[0]] = both[:half]
            gvl_bf[h, rows[0]] = both[half:].astype(BF)
            cross_a[h] = cross_c
            gvl_s[h] = nn(k2, above(c_hi, c_lo))
            gkl_s[h] = nt(beside(v, v), beside(c_hi, c_lo))
        else:
            k2, v = k2_s[0, h, :half], vc_s[0, h, :half]
            gv[h, rows[1]] = both[:half]
            gvl_bf[h, rows[1]] = (gvl_s[h] + both[half:]).astype(BF)
            cross[h] = (cross_a[h] + cross_c).astype(BF)
            gv_more[h] = nn(k2, above(c_hi, c_lo))
            gk_more[h] = nt(beside(v, v), beside(c_hi, c_lo))

    def key_part(c, h, which):
        y_hi, y_lo = split(y_s[c][h])
        part = slice(0, half) if which == 0 else slice(half, tok)
        scores = nn(k2_s[c, h, part], above(y_hi, y_lo))
        own = own_mask(half)
        scores = jnp.where(own, scores, 0.0) if which == 0 else jnp.where(own, 0.0, scores)
        a2_hi, a2_lo = split(vs_s[c, h, part] - scores)
        x_hi, x_lo = xs_s[h, rows[c], :DH], xs_s[h, rows[c], DH:]
        a1 = a1_s[c, h, part]
        g = nn(beside(a2_hi, a2_lo), above(x_hi, x_hi)) + nn(a2_hi, x_lo)
        return g - nt(a1, beside(y_hi, y_hi)) - nt(a1[:, :half], y_lo)

    def sym_part(c, h):
        y_hi, y_lo = split(-y_s[c][h])
        pair = nt(xt_s[c, h], beside(y_hi, y_hi)) + nt(xt_s[c, h, :, :half], y_lo)
        return pair + pair.T

    loop = ITERS // 2
    share = -(-heads // loop)

    def per_head(work):
        def run(i):
            for q in range(share):
                work(jnp.minimum(i * share + q, heads - 1) if share * loop > heads else i * share + q)
        return run

    def iterate(c, trips, extra):
        def step(i, carry):
            ps, pcs, sms, scs = [], [], [], []
            for h in range(heads):
                p = p_s[h]
                p_hi, p_lo = split(p)
                scs.append(nn(k2_s[c, h], above(p_hi, p_lo)))
                sms.append(nn(g_s[c, h], above(p_hi, p_lo)))
            images, curves = [], []
            for h in range(heads):
                p = p_s[h]
                scores = window_masked(scs[h])
                smooth = sms[h] + ridge[h] * p
                curve = jnp.sum(scores * scores, axis=0, keepdims=True)
                curves.append(curve + jnp.sum(p * smooth, axis=0, keepdims=True))
                images.append(nn(kt_s[c, h], scores.astype(BF)) + smooth)
            for h in range(heads):
                p = p_s[h]
                rr = rr_s[h]
                alpha = rr / (curves[h] + EPSILON)
                y_s[c][h] = y_s[c][h] + alpha * p
                r = r_s[h] - alpha * images[h]
                r_s[h] = r
                nr = jnp.sum(r * r, axis=0, keepdims=True)
                p_s[h] = r + nr / (rr + EPSILON) * p
                rr_s[h] = nr
            extra(i)
            return carry

        lax.fori_loop(0, trips, step, 0)

    def first_a(h):
        lag_scores(0, h)
        cross_part(0, h)

    def second_a(h):
        lag_scores(1, h)

    def first_b(h):
        cross_part(1, h)
        gkl_bf[h, rows[0]] = key_part(0, h, 1).astype(BF)

    def second_b(h):
        sy = sym_part(0, h)
        sym_a[h] = sy
        gkl_s[h] = gkl_s[h] + nn(k2_s[1, h, half:], above(*split(sy)))
        gk[h, rows[0]] = key_part(0, h, 0)
        gq[h, rows[0]] = y_s[0][h].T

    first, second = pl.ds(0, half), pl.ds(half, half)
    begin(0)
    iterate(0, loop, per_head(first_a))
    gva_hop = Hop(gvl_bf.at[:, first], gvl_in.at[:, first], -span).start()
    iterate(0, ITERS - loop, per_head(second_a))
    project(1)
    begin(1)
    iterate(1, loop, per_head(first_b))
    gvb_hop = Hop(gvl_bf.at[:, second], gvl_in.at[:, second], -span).start()
    cross_hops = mids(cross, cross_in, -1)
    gka_hop = Hop(gkl_bf.at[:, first], gkl_in.at[:, first], -span).start()
    iterate(1, ITERS - loop, per_head(second_b))
    for h in range(heads):
        gkl_bf[h, rows[1]] = (gkl_s[h] + key_part(1, h, 1)).astype(BF)
    gkb_hop = Hop(gkl_bf.at[:, second], gkl_in.at[:, second], -span).start()
    for h in range(heads):
        sy = sym_part(1, h)
        sym[h] = (sym_a[h] + sy).astype(BF)
        sym_a[h] = sy
    sym_hops = mids(sym, sym_in, -1)
    for h in range(heads):
        gk[h, rows[1]] = key_part(1, h, 0)
        more = gk_more[h] + nn(k2_s[0, h, :half], above(*split(sym_a[h])))
        gk[h, rows[0]] = gk[h, rows[0]] + more
        gv[h, rows[0]] = gv[h, rows[0]] + gv_more[h]
        gq[h, rows[1]] = y_s[1][h].T
    for hop in [gva_hop, gvb_hop] + cross_hops:
        hop.arrive()
    for h in range(heads):
        v_add = gvl_in[h].astype(F32)
        if span > 1:
            k, v = key[:, cols(h)], val[:, cols(h)]
            c_hi, c_lo = split(slots_sum(cross_in, h))
            v_add = v_add + nn(beside(k, k), above(c_hi, c_lo))
            gk[h] = gk[h] + nt(beside(v, v), beside(c_hi, c_lo))
        gv[h] = gv[h] + v_add
    for hop in [gka_hop, gkb_hop] + sym_hops:
        hop.arrive()
    for h in range(heads):
        k_add = gkl_in[h].astype(F32)
        if span > 1:
            k = key[:, cols(h)]
            k_add = k_add + nn(beside(k, k), above(*split(slots_sum(sym_in, h))))
        gk[h] = gk[h] + k_add
    for j in range(n_head):
        for c in range(2):
            pl.when(jnp.logical_and(has_right, j <= me))(lambda: d_copy(j, c, 1).wait_send())
            pl.when(jnp.logical_and(has_left, j >= me))(lambda: d_copy(j, c, -1).wait_send())
    for hop in hops:
        hop.finish()


def store(gq, gk, gv, gq_hbm, gk_hbm, gv_hbm, sem):
    copies = []
    for i, (source, target) in enumerate([(gq, gq_hbm), (gk, gk_hbm), (gv, gv_hbm)]):
        for h in range(source.shape[0]):
            copies.append(pltpu.make_async_copy(
                source.at[h], target.at[:, pl.ds(h * DH, DH)], sem.at[i, h]
            ))
    for copy in copies:
        copy.start()
    for copy in copies:
        copy.wait()


def body(key_rows, values, d_layer, out_weight, saved_solutions, ridge_scale):
    tok, cols = key_rows.shape
    heads = cols // DH
    half = tok // 2
    n_seq, n_head = lax.axis_size("seq"), lax.axis_size("head")
    span = n_seq // 4
    slots = max(span - 1, 1)
    copies = 6 + (4 if span == 2 else 3 * (span - 1))
    vmem = pl.BlockSpec(memory_space=pltpu.VMEM)
    hbm = pl.BlockSpec(memory_space=pltpu.HBM)
    flat = jax.ShapeDtypeStruct((tok, cols), F32)
    kept = pltpu.VMEM((heads, tok, DH), F32)
    rows_bf = pltpu.VMEM((tok, cols), BF)
    head_bf = pltpu.VMEM((heads, tok, DH), BF)
    mat_bf = pltpu.VMEM((heads, DH, DH), BF)
    mats_bf = pltpu.VMEM((heads, DH, 2 * DH), BF)
    mat_f = pltpu.VMEM((heads, DH, DH), F32)
    part_f = pltpu.VMEM((heads, half, DH), F32)
    vec = pltpu.VMEM((heads, DH, half), F32)
    results = pl.pallas_call(
        functools.partial(mega, span, n_seq, n_head),
        name="layer",
        out_shape=[kept, kept, kept],
        in_specs=[hbm] * 6,
        out_specs=[vmem, vmem, vmem],
        scratch_shapes=[
            pltpu.SMEM((heads,), F32), rows_bf, rows_bf, pltpu.VMEM((n_head,) + d_layer.shape, BF),
            pltpu.VMEM(out_weight.shape, BF), pltpu.VMEM((tok, cols), F32), rows_bf, rows_bf, head_bf,
            mats_bf, mats_bf, pltpu.VMEM((slots, heads, DH, 2 * DH), BF), mat_bf, mat_bf,
            pltpu.VMEM((slots, heads, DH, DH), BF), pltpu.VMEM((slots, heads, DH, DH), BF),
            head_bf, head_bf, head_bf, head_bf, part_f, part_f, part_f, part_f, mat_f, mat_f,
            pltpu.VMEM((2, heads, tok, 2 * DH), BF),
            pltpu.VMEM((2, heads, DH, tok), BF),
            pltpu.VMEM((2, heads, tok, DH), BF),
            pltpu.VMEM((heads, tok, 2 * DH), BF),
            pltpu.VMEM((2, heads, DH, tok), BF),
            pltpu.VMEM((2, heads, tok, tok), BF),
            pltpu.VMEM((2, heads, tok, half), F32),
            pltpu.VMEM((2, heads, DH, 2 * DH), F32),
            pltpu.VMEM((2, heads, DH, 2 * DH), BF),
            pltpu.VMEM((2, heads, DH, 2 * DH), BF),
            vec, vec, vec, vec,
            pltpu.VMEM((heads, 1, half), F32),
            pltpu.SemaphoreType.DMA((6,)),
            pltpu.SemaphoreType.DMA((4 * n_head,)),
            pltpu.SemaphoreType.DMA((2 * n_head,)),
            pltpu.SemaphoreType.DMA((copies,)),
            pltpu.SemaphoreType.DMA((copies,)),
        ],
        compiler_params=pltpu.CompilerParams(
            collective_id=0, has_side_effects=True, vmem_limit_bytes=48 * 1024 * 1024
        ),
    )(*(
        pltpu.with_memory_space_constraint(array, pltpu.HBM)
        for array in (ridge_scale, key_rows, values, d_layer, out_weight, saved_solutions)
    ))
    return pl.pallas_call(
        store,
        name="store",
        out_shape=[flat, flat, flat],
        in_specs=[vmem, vmem, vmem],
        out_specs=[hbm, hbm, hbm],
        scratch_shapes=[pltpu.SemaphoreType.DMA((3, heads))],
        compiler_params=pltpu.CompilerParams(vmem_limit_bytes=8 * 1024 * 1024),
    )(*(pltpu.with_memory_space_constraint(result, pltpu.VMEM) for result in results))


def solution(mesh):
    return jax.shard_map(
        body,
        mesh=mesh,
        in_specs=(
            P("seq", "head"),
            P("seq", "head"),
            P("seq", "head"),
            P("head", None),
            P("seq", "head"),
            P("head"),
        ),
        out_specs=(P("seq", "head"), P("seq", "head"), P("seq", "head")),
        check_vma=False,
    )
```

```python
import functools
import jax
import jax.numpy as jnp
from jax import lax
from jax.experimental import pallas as pl
from jax.experimental.pallas import tpu as pltpu
from jax.sharding import PartitionSpec as P

DH = 128
ITERS = 8
PIECES = 4
EPSILON = 1e-06
BF = jnp.bfloat16
F32 = jnp.float32
MESH = pl.DeviceIdType.MESH


def nn(left, right):
    return lax.dot_general(left, right, (((1,), (0,)), ((), ())), preferred_element_type=F32)


def nt(left, right):
    return lax.dot_general(left, right, (((1,), (1,)), ((), ())), preferred_element_type=F32)


def split(a):
    hi = a.astype(BF)
    return hi, (a - hi.astype(F32)).astype(BF)


def flip(a):
    return a.astype(F32).T.astype(BF)


def beside(*parts):
    return jnp.concatenate(parts, axis=1)


def above(*parts):
    return jnp.concatenate(parts, axis=0)


def own_mask(tok):
    key_ids = lax.broadcasted_iota(jnp.int32, (tok, tok), 0)
    tok_ids = lax.broadcasted_iota(jnp.int32, (tok, tok), 1)
    return key_ids <= tok_ids


def window_masked(scores):
    tok = scores.shape[1]
    own = own_mask(tok)
    return above(jnp.where(own, scores[:tok], 0.0), jnp.where(own, 0.0, scores[tok:]))


def slots_sum(ref, h):
    total = ref[0, h].astype(F32)
    for slot in range(1, ref.shape[0]):
        total = total + ref[slot, h].astype(F32)
    return total


def mega(span, n_seq, n_head, ridge_hbm, key_hbm, val_hbm, d_hbm, w_hbm, sav_hbm, gq, gk, gv,
         ridge, key, val, d_all, w, sav, key_lag, val_lag, ot_s,
         mid, mid_lag, mid_in, cross, sym, cross_lead, sym_lead, cross_in, sym_in,
         x_bf, x_lead, o_lead, y_bf, y_lead,
         k2_s, kt_s, vc_s, xs_s, xt_s, a1_s, vs_s, full_s, g_s, st_s, r_s, p_s, ya_s, yb_s, rr_s,
         local_sem, dsend_sem, drecv_sem, send_sem, recv_sem):
    s = lax.axis_index("seq")
    me = lax.axis_index("head")
    heads = ridge.shape[0]
    tok = key.shape[0]
    half = tok // 2
    width = d_all.shape[2]
    rows = [slice(0, half), slice(half, tok)]
    pieces = [range(0, PIECES // 2), range(PIECES // 2, PIECES)]
    y_s = [ya_s, yb_s]
    d_copy_in = pltpu.make_async_copy(d_hbm, d_all.at[me], local_sem.at[0])
    key_copy = pltpu.make_async_copy(key_hbm, key, local_sem.at[1])
    val_copy = pltpu.make_async_copy(val_hbm, val, local_sem.at[2])
    w_copy = pltpu.make_async_copy(w_hbm, w, local_sem.at[3])
    x_copy = pltpu.make_async_copy(sav_hbm, sav, local_sem.at[4])
    ridge_copy = pltpu.make_async_copy(ridge_hbm, ridge, local_sem.at[5])
    for copy in (d_copy_in, key_copy, val_copy, x_copy, w_copy, ridge_copy):
        copy.start()

    def exists(d):
        return s + d < n_seq if d > 0 else s + d >= 0

    barrier = pltpu.get_barrier_semaphore()
    has_right, has_left = me + 1 < n_head, me > 0
    for there, step in ((has_right, 1), (has_left, -1)):
        @pl.when(there)
        def _():
            pl.semaphore_signal(barrier, inc=1, device_id={"head": me + step}, device_id_type=MESH)
    for d in [d for m in range(1, span + 1) for d in (m, -m)]:
        @pl.when(exists(d))
        def _():
            pl.semaphore_signal(barrier, inc=1, device_id={"seq": s + d}, device_id_type=MESH)
    pl.semaphore_wait(
        barrier,
        jnp.minimum(me, 1) + jnp.minimum(n_head - 1 - me, 1)
        + jnp.minimum(s, span) + jnp.minimum(n_seq - 1 - s, span),
    )

    counter = [0]
    hops = []

    class Hop:
        def __init__(self, source, target, d, sender=None, receiver=None):
            self.sender = exists(d) if sender is None else sender
            self.receiver = exists(-d) if receiver is None else receiver
            self.copy = pltpu.make_async_remote_copy(
                src_ref=source,
                dst_ref=target,
                send_sem=send_sem.at[counter[0]],
                recv_sem=recv_sem.at[counter[0]],
                device_id={"seq": s + d},
                device_id_type=MESH,
            )
            counter[0] += 1
            hops.append(self)
            if receiver is None:
                @pl.when(jnp.logical_not(self.receiver))
                def _():
                    target[...] = jnp.zeros(target.shape, target.dtype)

        def start(self):
            pl.when(self.sender)(self.copy.start)
            return self

        def arrive(self):
            pl.when(self.receiver)(self.copy.wait_recv)

        def finish(self):
            pl.when(self.sender)(self.copy.wait_send)

    def mids(source, target, sign):
        return [Hop(source, target.at[m - 1], sign * m).start() for m in range(1, span)]

    def d_copy(origin, q, step):
        piece = d_all.at[origin, pl.ds(q * (tok // PIECES), tok // PIECES)]
        place = origin * PIECES + q
        return pltpu.make_async_remote_copy(
            src_ref=piece,
            dst_ref=piece,
            send_sem=dsend_sem.at[place + (0 if step > 0 else PIECES * n_head)],
            recv_sem=drecv_sem.at[place],
            device_id={"head": me + step},
            device_id_type=MESH,
        )

    def d_start(q):
        pl.when(has_right)(lambda: d_copy(me, q, 1).start())
        pl.when(has_left)(lambda: d_copy(me, q, -1).start())

    def d_relay(k, q):
        @pl.when(jnp.logical_and(me - k >= 0, has_right))
        def _():
            copy = d_copy(me - k, q, 1)
            copy.wait_recv()
            copy.start()

        @pl.when(jnp.logical_and(me + k < n_head, has_left))
        def _():
            copy = d_copy(me + k, q, -1)
            copy.wait_recv()
            copy.start()

    at_end = jnp.logical_or(me == 0, me == n_head - 1)

    def project(c):
        acc = None
        for i in range(n_head):
            origin = jnp.where(me == 0, i, n_head - 1 - i)
            if i:
                @pl.when(at_end)
                def _():
                    for q in pieces[c]:
                        d_copy(origin, q, 1).wait_recv()
            col = pl.multiple_of(origin * width, width)
            part = nt(w[:, pl.ds(col, width)], d_all[origin, rows[c]])
            acc = part if acc is None else acc + part
        for h in range(heads):
            ot_s[c, h] = acc[h * DH : (h + 1) * DH].astype(BF)

    def cols(h):
        return slice(h * DH, (h + 1) * DH)

    d_copy_in.wait()
    for q in pieces[0]:
        d_start(q)
    key_copy.wait()
    key_hop = Hop(key, key_lag, span).start()
    val_copy.wait()
    val_hop = Hop(val, val_lag, span).start()
    for h in range(heads):
        total = None
        for c in range(2):
            k, v = key[rows[c], cols(h)], val[rows[c], cols(h)]
            kt = flip(k)
            kt_s[c, h, :, :half] = kt
            k2_s[c, h, :half] = beside(k, k)
            vc_s[c, h, :half] = v
            both = nn(kt, beside(k, v))
            if c == 0:
                full_s[1, h] = both
            total = both if total is None else total + both
        mid[h] = total.astype(BF)
    paired = span == 2
    if paired:
        odd = lax.rem(s, 2) == 1
        even = jnp.logical_not(odd)
        mid_hops = [Hop(mid, mid_in.at[0], 1, even, odd).start()]
    else:
        mid_hops = mids(mid, mid_in, 1)
    x_copy.wait()
    for h in range(heads):
        x_hi, x_lo = split(sav[:, cols(h)])
        x_bf[h] = x_hi
        xs_s[h] = beside(x_hi, x_lo)
    x_hop = Hop(x_bf, x_lead, -span).start()
    for h in range(heads):
        for c in range(2):
            xt_s[c, h] = beside(*split(sav[rows[c], cols(h)].T))
            scores = nt(k2_s[c, h, :half], xs_s[h, rows[c]])
            a1_s[c, h] = beside(*split(jnp.where(own_mask(half), scores, 0.0)))
    late = list(pieces[1])
    for k in range(1, max(n_head - 1, len(late) + 1)):
        if k < n_head - 1:
            for q in pieces[0]:
                d_relay(k, q)
        if late:
            d_start(late.pop(0))
    if n_head > 2:
        for q in pieces[1]:
            d_relay(1, q)
    w_copy.wait()
    ridge_copy.wait()
    project(0)
    key_hop.arrive()
    for h in range(heads):
        for c in range(2):
            k = key_lag[rows[c], cols(h)]
            kt_s[c, h, :, half:] = flip(k)
            k2_s[c, h, half:] = beside(k, k)
    val_hop.arrive()
    for h in range(heads):
        for c in range(2):
            vc_s[c, h, half:] = val_lag[rows[c], cols(h)]
        late = nn(kt_s[1, h, :, half:], beside(k2_s[1, h, half:, :DH], vc_s[1, h, half:]))
        full_s[0, h] = late
        if paired:
            early = nn(kt_s[0, h, :, half:], beside(k2_s[0, h, half:, :DH], vc_s[0, h, half:]))
            mid_lag[h] = (early + late).astype(BF)
    if paired:
        mid_hops.append(Hop(mid_lag, mid_in.at[0], -1, odd, even).start())
    for k in range(2, n_head - 1):
        for q in pieces[1]:
            d_relay(k, q)
    pl.when(jnp.logical_not(at_end))(lambda: project(1))
    for hop in mid_hops:
        hop.arrive()
    for h in range(heads):
        for c in range(2):
            total = full_s[c, h]
            if span > 1:
                total = total + slots_sum(mid_in, h)
            g_hi, g_lo = split(total[:, :DH])
            g_s[c, h] = beside(g_hi, g_hi)
            st_s[c, h] = beside(*split(total[:, DH:]))

    def begin(c):
        outs = [ot_s[c, h] for h in range(heads)]
        scores = [nn(vc_s[c, h], outs[h]) for h in range(heads)]
        base = [nn(st_s[c, h], above(outs[h], outs[h])) for h in range(heads)]
        parts = []
        for h in range(heads):
            masked = window_masked(scores[h])
            vs_s[c, h] = masked[:half]
            parts.append(split(masked))
        rs = [base[h] + nn(kt_s[c, h], parts[h][0]) + nn(kt_s[c, h], parts[h][1]) for h in range(heads)]
        for h in range(heads):
            r_s[h] = rs[h]
            p_s[h] = rs[h]
            y_s[c][h] = jnp.zeros_like(rs[h])
            rr_s[h] = jnp.sum(rs[h] * rs[h], axis=0, keepdims=True)

    def iterate(c):
        def step(i, carry):
            smooths, scores = [], []
            for h in range(heads):
                p_hi, p_lo = split(p_s[h])
                p2 = above(p_hi, p_lo)
                scores.append(nn(k2_s[c, h], p2))
                smooths.append(nn(g_s[c, h], p2))
            images, curves = [], []
            for h in range(heads):
                p = p_s[h]
                masked = window_masked(scores[h])
                smooth = smooths[h] + ridge[h] * p
                curve = jnp.sum(masked * masked, axis=0, keepdims=True)
                curves.append(curve + jnp.sum(p * smooth, axis=0, keepdims=True))
                images.append(nn(kt_s[c, h], masked.astype(BF)) + smooth)
            for h in range(heads):
                p = p_s[h]
                rr = rr_s[h]
                alpha = rr / (curves[h] + EPSILON)
                y_s[c][h] = y_s[c][h] + alpha * p
                r = r_s[h] - alpha * images[h]
                r_s[h] = r
                nr = jnp.sum(r * r, axis=0, keepdims=True)
                p_s[h] = r + nr / (rr + EPSILON) * p
                rr_s[h] = nr
            return carry

        lax.fori_loop(0, ITERS, step, 0)
        for h in range(heads):
            y_bf[c, h] = y_s[c][h].astype(BF)

    every = list(range(heads))

    def twice(a):
        return beside(a, a)

    def negative_sym(pair):
        return -(pair + pair.T)

    def apply_states(c_f, s_f, k, v):
        c_hi, c_lo = split(c_f)
        to_k = nt(twice(v), beside(c_hi, c_lo))
        if s_f is not None:
            to_k = to_k + nn(twice(k), above(*split(s_f)))
        return to_k, nn(twice(k), above(c_hi, c_lo))

    o_hops = [Hop(ot_s.at[0], o_lead.at[0], -span).start()]
    begin(0)
    iterate(0)
    y_hops = [Hop(y_bf.at[0], y_lead.at[0], -span).start()]
    pl.when(at_end)(lambda: project(1))
    o_hops.append(Hop(ot_s.at[1], o_lead.at[1], -span).start())
    begin(1)
    iterate(1)
    y_hops.append(Hop(y_bf.at[1], y_lead.at[1], -span).start())

    crosses = [[nt(xt_s[c, h], twice(ot_s[c, h])) for h in every] for c in range(2)]
    pairs = [[], []]
    for c in range(2):
        for h in every:
            y_hi, y_lo = split(y_s[c][h])
            pairs[c].append(nt(xt_s[c, h], twice(y_hi)) + nt(xt_s[c, h, :, :half], y_lo))
    for h in every:
        cross[h] = (crosses[0][h] + crosses[1][h]).astype(BF)
        sym[h] = negative_sym(pairs[0][h] + pairs[1][h]).astype(BF)
    if paired:
        state_hops = [
            Hop(cross, cross_in.at[0], -1, odd, even).start(), Hop(sym, sym_in.at[0], -1, odd, even).start()
        ]
    else:
        state_hops = mids(cross, cross_in, -1) + mids(sym, sym_in, -1)
    for h in every:
        to_k, to_v = apply_states(
            crosses[1][h], negative_sym(pairs[1][h]), k2_s[0, h, :half, :DH], vc_s[0, h, :half]
        )
        gk[h, rows[0]] = to_k
        gv[h, rows[0]] = to_v + nt(a1_s[0, h], twice(ot_s[0, h]))
        gv[h, rows[1]] = nt(a1_s[1, h], twice(ot_s[1, h]))
    own = own_mask(half)
    for c in range(2):
        ys = [split(y_s[c][h]) for h in every]
        scores = [nn(k2_s[c, h, :half], above(*ys[h])) for h in every]
        for h in every:
            y_hi, y_lo = ys[h]
            a2_hi, a2_lo = split(vs_s[c, h] - jnp.where(own, scores[h], 0.0))
            x_hi, x_lo = xs_s[h, rows[c], :DH], xs_s[h, rows[c], DH:]
            a1 = a1_s[c, h]
            g = nn(beside(a2_hi, a2_lo), above(x_hi, x_hi)) + nn(a2_hi, x_lo)
            g = g - nt(a1, twice(y_hi)) - nt(a1[:, :half], y_lo)
            gk[h, rows[c]] = gk[h, rows[c]] + g if c == 0 else g
    for h in every:
        for c in range(2):
            gq[h, rows[c]] = y_s[c][h].T

    x_hop.arrive()
    for hop in o_hops:
        hop.arrive()
    seen = []
    for c in range(2):
        scores = [nt(k2_s[c, h, :half, :DH], x_lead[h, rows[c]]) for h in every]
        seen.append([beside(*split(jnp.where(own, 0.0, t))) for t in scores])
        for h in every:
            gv[h, rows[c]] = gv[h, rows[c]] + nt(seen[c][h], twice(o_lead[c, h]))
    flipped = [[flip(x_lead[h, rows[c]]) for h in every] for c in range(2)]
    crosses = [[nt(flipped[c][h], o_lead[c, h]) for h in every] for c in range(2)]
    if paired:
        for h in every:
            cross_lead[h] = (crosses[0][h] + crosses[1][h]).astype(BF)
        state_hops.append(Hop(cross_lead, cross_in.at[0], 1, even, odd).start())

    def lead_part(c):
        scores = []
        for h in every:
            vk = beside(vc_s[c, h, :half], k2_s[c, h, :half, :DH])
            scores.append(nn(vk, above(o_lead[c, h], -y_lead[c, h])))
        for h in every:
            a2_hi, a2_lo = split(jnp.where(own, 0.0, scores[h]))
            x = x_lead[h, rows[c]]
            g = nn(beside(a2_hi, a2_lo), above(x, x)) - nt(seen[c][h], twice(y_lead[c, h]))
            gk[h, rows[c]] = gk[h, rows[c]] + g

    y_hops[0].arrive()
    pairs = [nt(flipped[0][h], y_lead[0, h]) for h in every]
    for h in every:
        to_k, to_v = apply_states(crosses[0][h], negative_sym(pairs[h]), k2_s[1, h, :half, :DH], vc_s[1, h, :half])
        gk[h, rows[1]] = gk[h, rows[1]] + to_k
        gv[h, rows[1]] = gv[h, rows[1]] + to_v
    lead_part(0)
    y_hops[1].arrive()
    if paired:
        lates = [nt(flipped[1][h], y_lead[1, h]) for h in every]
        for h in every:
            sym_lead[h] = negative_sym(pairs[h] + lates[h]).astype(BF)
        state_hops.append(Hop(sym_lead, sym_in.at[0], 1, even, odd).start())
    lead_part(1)
    for hop in state_hops:
        hop.arrive()
    if span > 1:
        for h in every:
            c_f, s_f = slots_sum(cross_in, h), slots_sum(sym_in, h)
            to_k, to_v = apply_states(c_f, s_f, key[:, cols(h)], val[:, cols(h)])
            gk[h] = gk[h] + to_k
            gv[h] = gv[h] + to_v
    for j in range(n_head):
        @pl.when(jnp.logical_and(has_right, j <= me))
        def _():
            for q in range(PIECES):
                d_copy(j, q, 1).wait_send()

        @pl.when(jnp.logical_and(has_left, j >= me))
        def _():
            for q in range(PIECES):
                d_copy(j, q, -1).wait_send()
    for hop in hops:
        hop.finish()


def store(gq, gk, gv, gq_hbm, gk_hbm, gv_hbm, sem):
    copies = []
    for i, (source, target) in enumerate([(gq, gq_hbm), (gk, gk_hbm), (gv, gv_hbm)]):
        for h in range(source.shape[0]):
            copies.append(pltpu.make_async_copy(
                source.at[h], target.at[:, pl.ds(h * DH, DH)], sem.at[i, h]
            ))
    for copy in copies:
        copy.start()
    for copy in copies:
        copy.wait()


def body(key_rows, values, d_layer, out_weight, saved_solutions, ridge_scale):
    tok, cols = key_rows.shape
    heads = cols // DH
    half = tok // 2
    n_seq, n_head = lax.axis_size("seq"), lax.axis_size("head")
    span = n_seq // 4
    slots = max(span - 1, 1)
    copies = 7 + (6 if span == 2 else 3 * (span - 1))
    vmem = pl.BlockSpec(memory_space=pltpu.VMEM)
    hbm = pl.BlockSpec(memory_space=pltpu.HBM)
    flat = jax.ShapeDtypeStruct((tok, cols), F32)
    kept = pltpu.VMEM((heads, tok, DH), F32)
    rows_bf = pltpu.VMEM((tok, cols), BF)
    head_bf = pltpu.VMEM((heads, tok, DH), BF)
    mat_bf = pltpu.VMEM((heads, DH, DH), BF)
    mats_bf = pltpu.VMEM((heads, DH, 2 * DH), BF)
    turned_bf = pltpu.VMEM((2, heads, DH, half), BF)
    vec = pltpu.VMEM((heads, DH, half), F32)
    results = pl.pallas_call(
        functools.partial(mega, span, n_seq, n_head),
        name="layer",
        out_shape=[kept, kept, kept],
        in_specs=[hbm] * 6,
        out_specs=[vmem, vmem, vmem],
        scratch_shapes=[
            pltpu.SMEM((heads,), F32), rows_bf, rows_bf, pltpu.VMEM((n_head,) + d_layer.shape, BF),
            pltpu.VMEM(out_weight.shape, BF), pltpu.VMEM((tok, cols), F32), rows_bf, rows_bf, turned_bf,
            mats_bf, mats_bf, pltpu.VMEM((slots, heads, DH, 2 * DH), BF), mat_bf, mat_bf, mat_bf, mat_bf,
            pltpu.VMEM((slots, heads, DH, DH), BF), pltpu.VMEM((slots, heads, DH, DH), BF),
            head_bf, head_bf, turned_bf, turned_bf, turned_bf,
            pltpu.VMEM((2, heads, tok, 2 * DH), BF),
            pltpu.VMEM((2, heads, DH, tok), BF),
            pltpu.VMEM((2, heads, tok, DH), BF),
            pltpu.VMEM((heads, tok, 2 * DH), BF),
            pltpu.VMEM((2, heads, DH, tok), BF),
            pltpu.VMEM((2, heads, half, tok), BF),
            pltpu.VMEM((2, heads, half, half), F32),
            pltpu.VMEM((2, heads, DH, 2 * DH), F32),
            pltpu.VMEM((2, heads, DH, 2 * DH), BF),
            pltpu.VMEM((2, heads, DH, 2 * DH), BF),
            vec, vec, vec, vec,
            pltpu.VMEM((heads, 1, half), F32),
            pltpu.SemaphoreType.DMA((6,)),
            pltpu.SemaphoreType.DMA((2 * PIECES * n_head,)),
            pltpu.SemaphoreType.DMA((PIECES * n_head,)),
            pltpu.SemaphoreType.DMA((copies,)),
            pltpu.SemaphoreType.DMA((copies,)),
        ],
        compiler_params=pltpu.CompilerParams(
            collective_id=0, has_side_effects=True, vmem_limit_bytes=48 * 1024 * 1024
        ),
    )(*(
        pltpu.with_memory_space_constraint(array, pltpu.HBM)
        for array in (ridge_scale, key_rows, values, d_layer, out_weight, saved_solutions)
    ))
    return pl.pallas_call(
        store,
        name="store",
        out_shape=[flat, flat, flat],
        in_specs=[vmem, vmem, vmem],
        out_specs=[hbm, hbm, hbm],
        scratch_shapes=[pltpu.SemaphoreType.DMA((3, heads))],
        compiler_params=pltpu.CompilerParams(vmem_limit_bytes=8 * 1024 * 1024),
    )(*(pltpu.with_memory_space_constraint(result, pltpu.VMEM) for result in results))


def solution(mesh):
    return jax.shard_map(
        body,
        mesh=mesh,
        in_specs=(
            P("seq", "head"),
            P("seq", "head"),
            P("seq", "head"),
            P("head", None),
            P("seq", "head"),
            P("head"),
        ),
        out_specs=(P("seq", "head"), P("seq", "head"), P("seq", "head")),
        check_vma=False,
    )
```

```python
import functools
import jax
import jax.numpy as jnp
from jax import lax
from jax.experimental import pallas as pl
from jax.experimental.pallas import tpu as pltpu
from jax.sharding import PartitionSpec as P

DH = 128
ITERS = 8
PIECES = 4
EPSILON = 1e-06
BF = jnp.bfloat16
F32 = jnp.float32
MESH = pl.DeviceIdType.MESH


def nn(left, right):
    return lax.dot_general(left, right, (((1,), (0,)), ((), ())), preferred_element_type=F32)


def nt(left, right):
    return lax.dot_general(left, right, (((1,), (1,)), ((), ())), preferred_element_type=F32)


def split(a):
    hi = a.astype(BF)
    return hi, (a - hi.astype(F32)).astype(BF)


def flip(a):
    return a.astype(F32).T.astype(BF)


def beside(*parts):
    return jnp.concatenate(parts, axis=1)


def above(*parts):
    return jnp.concatenate(parts, axis=0)


def own_mask(tok):
    key_ids = lax.broadcasted_iota(jnp.int32, (tok, tok), 0)
    tok_ids = lax.broadcasted_iota(jnp.int32, (tok, tok), 1)
    return key_ids <= tok_ids


def window_masked(scores):
    tok = scores.shape[1]
    own = own_mask(tok)
    return above(jnp.where(own, scores[:tok], 0.0), jnp.where(own, 0.0, scores[tok:]))


def slots_sum(ref, h):
    total = ref[0, h].astype(F32)
    for slot in range(1, ref.shape[0]):
        total = total + ref[slot, h].astype(F32)
    return total


def mega(span, n_seq, n_head, ridge_hbm, key_hbm, val_hbm, d_hbm, w_hbm, sav_hbm, gq, gk, gv, key_out, sym_out,
         ridge, key, val, d_all, w, sav, key_lag, val_lag, ot_s,
         mid, mid_lag, mid_in, cross, sym, cross_lead, sym_lead, cross_in, sym_in,
         x_bf, x_lead, o_lead, y_bf, y_lead, key_stop, val_stop, x_stop, o_stop,
         k2_s, kt_s, vc_s, xs_s, xt_s, a1_s, vs_s, full_s, g_s, st_s, r_s, p_s, p2_s, ya_s, yb_s, rr_s,
         local_sem, dsend_sem, drecv_sem, send_sem, recv_sem):
    s = lax.axis_index("seq")
    me = lax.axis_index("head")
    heads = ridge.shape[0]
    tok = key.shape[0]
    half = tok // 2
    width = d_all.shape[2]
    rows = [slice(0, half), slice(half, tok)]
    pieces = [range(0, PIECES // 2), range(PIECES // 2, PIECES)]
    y_s = [ya_s, yb_s]
    d_copy_in = pltpu.make_async_copy(d_hbm, d_all.at[me], local_sem.at[0])
    key_copy = pltpu.make_async_copy(key_hbm, key, local_sem.at[1])
    val_copy = pltpu.make_async_copy(val_hbm, val, local_sem.at[2])
    w_copy = pltpu.make_async_copy(w_hbm, w, local_sem.at[3])
    x_copy = pltpu.make_async_copy(sav_hbm, sav, local_sem.at[4])
    ridge_copy = pltpu.make_async_copy(ridge_hbm, ridge, local_sem.at[5])
    for copy in (d_copy_in, key_copy, val_copy, x_copy, w_copy, ridge_copy):
        copy.start()

    def exists(d):
        return s + d < n_seq if d > 0 else s + d >= 0

    paired = span == 2
    odd = lax.rem(s, 2) == 1
    even = jnp.logical_not(odd)
    detour = paired and n_seq == 8
    barrier = pltpu.get_barrier_semaphore()
    has_right, has_left = me + 1 < n_head, me > 0
    for there, step in ((has_right, 1), (has_left, -1)):
        @pl.when(there)
        def _():
            pl.semaphore_signal(barrier, inc=1, device_id={"head": me + step}, device_id_type=MESH)
    for d in [d for m in range(1, span + 1) for d in (m, -m)]:
        @pl.when(exists(d))
        def _():
            pl.semaphore_signal(barrier, inc=1, device_id={"seq": s + d}, device_id_type=MESH)
    if detour:
        @pl.when(odd)
        def _():
            far = lax.rem(s + n_seq // 2, n_seq)
            pl.semaphore_signal(barrier, inc=1, device_id={"seq": far}, device_id_type=MESH)
    pl.semaphore_wait(
        barrier,
        (lax.rem(s, 2) if detour else 0) +
        jnp.minimum(me, 1) + jnp.minimum(n_head - 1 - me, 1)
        + jnp.minimum(s, span) + jnp.minimum(n_seq - 1 - s, span),
    )

    counter = [0]
    hops = []

    class Hop:
        def __init__(self, source, target, d, sender=None, receiver=None, skip=None):
            self.sender = exists(d) if sender is None else sender
            self.receiver = exists(-d) if receiver is None else receiver
            if skip is not None:
                self.sender = jnp.logical_and(self.sender, s != skip[0])
                self.receiver = jnp.logical_and(self.receiver, s != skip[1])
            self.copy = pltpu.make_async_remote_copy(
                src_ref=source,
                dst_ref=target,
                send_sem=send_sem.at[counter[0]],
                recv_sem=recv_sem.at[counter[0]],
                device_id={"seq": s + d},
                device_id_type=MESH,
            )
            counter[0] += 1
            hops.append(self)
            if receiver is None:
                @pl.when(jnp.logical_not(exists(-d)))
                def _():
                    target[...] = jnp.zeros(target.shape, target.dtype)

        def start(self):
            pl.when(self.sender)(self.copy.start)
            return self

        def arrive(self):
            pl.when(self.receiver)(self.copy.wait_recv)

        def finish(self):
            pl.when(self.sender)(self.copy.wait_send)

    class Route:
        def __init__(self, source, target, d, stop):
            a, b = n_seq // 2 - d // 2, n_seq // 2 + d // 2
            way = (a + n_seq // 2) % n_seq
            self.direct = Hop(source, target, d, skip=(a, b) if detour else None).start()
            self.legs = []
            if detour:
                self.legs = [
                    Hop(source, stop, way - a, s == a, s == way).start(),
                    Hop(stop, target, b - way, s == way, s == b),
                ]

        def forward(self):
            if self.legs:
                self.legs[0].arrive()
                self.legs[1].start()

        def arrive(self):
            self.direct.arrive()
            if self.legs:
                self.legs[1].arrive()

    def mids(source, target, sign):
        return [Hop(source, target.at[m - 1], sign * m).start() for m in range(1, span)]

    def d_copy(origin, q, step):
        piece = d_all.at[origin, pl.ds(q * (tok // PIECES), tok // PIECES)]
        place = origin * PIECES + q
        return pltpu.make_async_remote_copy(
            src_ref=piece,
            dst_ref=piece,
            send_sem=dsend_sem.at[place + (0 if step > 0 else PIECES * n_head)],
            recv_sem=drecv_sem.at[place],
            device_id={"head": me + step},
            device_id_type=MESH,
        )

    def d_start(q):
        pl.when(has_right)(lambda: d_copy(me, q, 1).start())
        pl.when(has_left)(lambda: d_copy(me, q, -1).start())

    def d_relay(k, q):
        @pl.when(jnp.logical_and(me - k >= 0, has_right))
        def _():
            copy = d_copy(me - k, q, 1)
            copy.wait_recv()
            copy.start()

        @pl.when(jnp.logical_and(me + k < n_head, has_left))
        def _():
            copy = d_copy(me + k, q, -1)
            copy.wait_recv()
            copy.start()

    at_end = jnp.logical_or(me == 0, me == n_head - 1)

    def project(c):
        acc = None
        for i in range(n_head):
            origin = jnp.where(me == 0, i, n_head - 1 - i)
            if i:
                @pl.when(at_end)
                def _():
                    for q in pieces[c]:
                        d_copy(origin, q, 1).wait_recv()
            col = pl.multiple_of(origin * width, width)
            part = nt(w[:, pl.ds(col, width)], d_all[origin, rows[c]])
            acc = part if acc is None else acc + part
        for h in range(heads):
            ot_s[c, h] = acc[h * DH : (h + 1) * DH].astype(BF)

    def cols(h):
        return slice(h * DH, (h + 1) * DH)

    d_copy_in.wait()
    for q in pieces[0]:
        d_start(q)
    key_copy.wait()
    key_hop = Route(key, key_lag, span, key_stop)
    val_copy.wait()
    val_hop = Route(val, val_lag, span, val_stop)
    for h in range(heads):
        total = None
        for c in range(2):
            k, v = key[rows[c], cols(h)], val[rows[c], cols(h)]
            kt = flip(k)
            kt_s[c, h, :, :half] = kt
            k2_s[c, h, :half] = beside(k, k)
            vc_s[c, h, :half] = v
            both = nn(kt, beside(k, v))
            if c == 0:
                full_s[1, h] = both
            total = both if total is None else total + both
        mid[h] = total.astype(BF)
    if paired:
        mid_hops = [Hop(mid, mid_in.at[0], 1, even, odd).start()]
    else:
        mid_hops = mids(mid, mid_in, 1)
    x_copy.wait()
    for h in range(heads):
        x_hi, x_lo = split(sav[:, cols(h)])
        x_bf[h] = x_hi
        xs_s[h] = beside(x_hi, x_lo)
    x_hop = Route(x_bf, x_lead, -span, x_stop)
    for h in range(heads):
        for c in range(2):
            xt_s[c, h] = beside(*split(sav[rows[c], cols(h)].T))
            scores = nt(k2_s[c, h, :half], xs_s[h, rows[c]])
            a1_s[c, h] = beside(*split(jnp.where(own_mask(half), scores, 0.0)))
    late = list(pieces[1])
    for k in range(1, max(n_head - 1, len(late) + 1)):
        if k < n_head - 1:
            for q in pieces[0]:
                d_relay(k, q)
        if late:
            d_start(late.pop(0))
        if k == 1:
            key_hop.forward()
    val_hop.forward()
    x_hop.forward()
    rest = [(k, q) for k in range(1, n_head - 1) for q in pieces[1]]
    for k, q in rest[:2]:
        d_relay(k, q)
    rest = rest[2:]
    for h in range(heads):
        key_out[h] = key[:, cols(h)]
    w_copy.wait()
    ridge_copy.wait()
    project(0)
    o_hops = [Route(ot_s.at[0], o_lead.at[0], -span, o_stop)]
    key_hop.arrive()
    for h in range(heads):
        for c in range(2):
            k = key_lag[rows[c], cols(h)]
            kt_s[c, h, :, half:] = flip(k)
            k2_s[c, h, half:] = beside(k, k)
    val_hop.arrive()
    for h in range(heads):
        for c in range(2):
            vc_s[c, h, half:] = val_lag[rows[c], cols(h)]
        late = nn(kt_s[1, h, :, half:], beside(k2_s[1, h, half:, :DH], vc_s[1, h, half:]))
        full_s[0, h] = late
        if paired:
            early = nn(kt_s[0, h, :, half:], beside(k2_s[0, h, half:, :DH], vc_s[0, h, half:]))
            mid_lag[h] = (early + late).astype(BF)
    if paired:
        mid_hops.append(Hop(mid_lag, mid_in.at[0], -1, odd, even).start())
    for k, q in rest[: len(rest) // 2]:
        d_relay(k, q)
    for hop in mid_hops:
        hop.arrive()
    for h in range(heads):
        for c in range(2):
            total = full_s[c, h]
            if span > 1:
                total = total + slots_sum(mid_in, h)
            g_hi, g_lo = split(total[:, :DH])
            g_s[c, h] = beside(g_hi, g_hi)
            st_s[c, h] = beside(*split(total[:, DH:]))

    def begin(c):
        outs = [ot_s[c, h] for h in range(heads)]
        scores = [nn(vc_s[c, h], outs[h]) for h in range(heads)]
        base = [nn(st_s[c, h], above(outs[h], outs[h])) for h in range(heads)]
        parts = []
        for h in range(heads):
            masked = window_masked(scores[h])
            vs_s[c, h] = masked[:half]
            parts.append(split(masked))
        rs = [base[h] + nn(kt_s[c, h], parts[h][0]) + nn(kt_s[c, h], parts[h][1]) for h in range(heads)]
        for h in range(heads):
            r_s[h] = rs[h]
            p_s[h] = rs[h]
            p2_s[h] = above(*split(rs[h]))
            y_s[c][h] = jnp.zeros_like(rs[h])
            rr_s[h] = jnp.sum(rs[h] * rs[h], axis=0, keepdims=True)

    def iterate(c, between=None):
        def curves():
            smooths, scores = [], []
            for h in range(heads):
                scores.append(nn(k2_s[c, h], p2_s[h]))
                smooths.append(nn(g_s[c, h], p2_s[h]))
            result = []
            for h in range(heads):
                p = p_s[h]
                masked = window_masked(scores[h])
                smooth = smooths[h] + ridge[h] * p
                curve = jnp.sum(masked * masked, axis=0, keepdims=True)
                curve = curve + jnp.sum(p * smooth, axis=0, keepdims=True)
                result.append((masked, smooth, curve + EPSILON))
            return result

        def step(i, carry):
            found = curves()
            images = [nn(kt_s[c, h], found[h][0].astype(BF)) + found[h][1] for h in range(heads)]
            for h in range(heads):
                p = p_s[h]
                rr = rr_s[h]
                alpha = rr / found[h][2]
                y_s[c][h] = y_s[c][h] + alpha * p
                r = r_s[h] - alpha * images[h]
                r_s[h] = r
                nr = jnp.sum(r * r, axis=0, keepdims=True)
                p = r + nr / (rr + EPSILON) * p
                p_s[h] = p
                p2_s[h] = above(*split(p))
                rr_s[h] = nr
            return carry

        if between is None:
            lax.fori_loop(0, ITERS - 1, step, 0)
        else:
            lax.fori_loop(0, ITERS // 2, step, 0)
            between()
            lax.fori_loop(ITERS // 2, ITERS - 1, step, 0)
        found = curves()
        for h in range(heads):
            y = y_s[c][h] + rr_s[h] / found[h][2] * p_s[h]
            y_s[c][h] = y
            y_bf[c, h] = y.astype(BF)

    every = list(range(heads))

    def twice(a):
        return beside(a, a)

    def negative_sym(pair):
        return -(pair + pair.T)

    def apply_states(c_f, s_f, k, v):
        c_hi, c_lo = split(c_f)
        to_k = nt(twice(v), beside(c_hi, c_lo))
        if s_f is not None:
            to_k = to_k + nn(twice(k), above(*split(s_f)))
        return to_k, nn(twice(k), above(c_hi, c_lo))

    def apply_cross():
        for h in every:
            to_k, to_v = apply_states(slots_sum(cross_in, h), None, key[:, cols(h)], val[:, cols(h)])
            gk[h] = gk[h] + to_k
            gv[h] = gv[h] + to_v

    def halfway():
        for k, q in rest[len(rest) // 2 :]:
            d_relay(k, q)
        o_hops[0].forward()

    begin(0)
    iterate(0, halfway)
    y_hops = [Hop(y_bf.at[0], y_lead.at[0], -span).start()]
    project(1)
    o_hops.append(Hop(ot_s.at[1], o_lead.at[1], -span).start())
    begin(1)
    iterate(1)
    y_hops.append(Hop(y_bf.at[1], y_lead.at[1], -span).start())

    crosses = [[nt(xt_s[c, h], twice(ot_s[c, h])) for h in every] for c in range(2)]
    pairs = [[], []]
    for c in range(2):
        for h in every:
            y_hi, y_lo = split(y_s[c][h])
            pairs[c].append(nt(xt_s[c, h], twice(y_hi)) + nt(xt_s[c, h, :, :half], y_lo))
    for h in every:
        cross[h] = (crosses[0][h] + crosses[1][h]).astype(BF)
        sym[h] = negative_sym(pairs[0][h] + pairs[1][h]).astype(BF)
    if paired:
        cross_hops = [Hop(cross, cross_in.at[0], -1, odd, even).start()]
        sym_hops = [Hop(sym, sym_in.at[0], -1, odd, even).start()]
    else:
        cross_hops, sym_hops = mids(cross, cross_in, -1), mids(sym, sym_in, -1)
    for h in every:
        to_k, to_v = apply_states(
            crosses[1][h], negative_sym(pairs[1][h]), k2_s[0, h, :half, :DH], vc_s[0, h, :half]
        )
        gk[h, rows[0]] = to_k
        gv[h, rows[0]] = to_v + nt(a1_s[0, h], twice(ot_s[0, h]))
        gv[h, rows[1]] = nt(a1_s[1, h], twice(ot_s[1, h]))
    own = own_mask(half)
    for c in range(2):
        ys = [split(y_s[c][h]) for h in every]
        scores = [nn(k2_s[c, h, :half], above(*ys[h])) for h in every]
        for h in every:
            y_hi, y_lo = ys[h]
            a2_hi, a2_lo = split(vs_s[c, h] - jnp.where(own, scores[h], 0.0))
            x_hi, x_lo = xs_s[h, rows[c], :DH], xs_s[h, rows[c], DH:]
            a1 = a1_s[c, h]
            g = nn(beside(a2_hi, a2_lo), above(x_hi, x_hi)) + nn(a2_hi, x_lo)
            g = g - nt(a1, twice(y_hi)) - nt(a1[:, :half], y_lo)
            gk[h, rows[c]] = gk[h, rows[c]] + g if c == 0 else g
    for h in every:
        for c in range(2):
            gq[h, rows[c]] = y_s[c][h].T

    x_hop.arrive()
    for hop in o_hops:
        hop.arrive()
    seen = []
    for c in range(2):
        scores = [nt(k2_s[c, h, :half, :DH], x_lead[h, rows[c]]) for h in every]
        seen.append([beside(*split(jnp.where(own, 0.0, t))) for t in scores])
        for h in every:
            gv[h, rows[c]] = gv[h, rows[c]] + nt(seen[c][h], twice(o_lead[c, h]))
    flipped = [[flip(x_lead[h, rows[c]]) for h in every] for c in range(2)]
    crosses = [[nt(flipped[c][h], o_lead[c, h]) for h in every] for c in range(2)]
    if paired:
        for h in every:
            cross_lead[h] = (crosses[0][h] + crosses[1][h]).astype(BF)
        cross_hops.append(Hop(cross_lead, cross_in.at[0], 1, even, odd).start())

    def lead_part(c):
        scores = []
        for h in every:
            vk = beside(vc_s[c, h, :half], k2_s[c, h, :half, :DH])
            scores.append(nn(vk, above(o_lead[c, h], -y_lead[c, h])))
        for h in every:
            a2_hi, a2_lo = split(jnp.where(own, 0.0, scores[h]))
            x = x_lead[h, rows[c]]
            g = nn(beside(a2_hi, a2_lo), above(x, x)) - nt(seen[c][h], twice(y_lead[c, h]))
            gk[h, rows[c]] = gk[h, rows[c]] + g

    y_hops[0].arrive()
    pairs = [nt(flipped[0][h], y_lead[0, h]) for h in every]
    for h in every:
        to_k, to_v = apply_states(crosses[0][h], negative_sym(pairs[h]), k2_s[1, h, :half, :DH], vc_s[1, h, :half])
        gk[h, rows[1]] = gk[h, rows[1]] + to_k
        gv[h, rows[1]] = gv[h, rows[1]] + to_v
    lead_part(0)
    for hop in cross_hops:
        hop.arrive()
    if span > 1:
        apply_cross()
    y_hops[1].arrive()
    if paired:
        lates = [nt(flipped[1][h], y_lead[1, h]) for h in every]
        for h in every:
            sym_lead[h] = negative_sym(pairs[h] + lates[h]).astype(BF)
        sym_hops.append(Hop(sym_lead, sym_in.at[0], 1, even, odd).start())
    lead_part(1)
    for hop in sym_hops:
        hop.arrive()
    for h in every:
        sym_out[h] = above(*split(slots_sum(sym_in, h))) if span > 1 else jnp.zeros(sym_out.shape[1:], BF)
    for j in range(n_head):
        @pl.when(jnp.logical_and(has_right, j <= me))
        def _():
            for q in range(PIECES):
                d_copy(j, q, 1).wait_send()

        @pl.when(jnp.logical_and(has_left, j >= me))
        def _():
            for q in range(PIECES):
                d_copy(j, q, -1).wait_send()
    for hop in hops:
        hop.finish()


def store(gq, gk, gv, key, sym, gq_hbm, gk_hbm, gv_hbm, total, sem):
    heads = gk.shape[0]

    def copies(i, source, target):
        return [
            pltpu.make_async_copy(source.at[h], target.at[:, pl.ds(h * DH, DH)], sem.at[i, h])
            for h in range(heads)
        ]

    early = copies(0, gq, gq_hbm) + copies(1, gv, gv_hbm)
    late = copies(2, total, gk_hbm)
    for copy in early:
        copy.start()
    for h in range(heads):
        k = key[h]
        total[h] = gk[h] + nn(beside(k, k), sym[h])
        late[h].start()
    for copy in early + late:
        copy.wait()


def body(key_rows, values, d_layer, out_weight, saved_solutions, ridge_scale):
    tok, cols = key_rows.shape
    heads = cols // DH
    half = tok // 2
    n_seq, n_head = lax.axis_size("seq"), lax.axis_size("head")
    span = n_seq // 4
    slots = max(span - 1, 1)
    copies = 15 + (6 if span == 2 else 3 * (span - 1))
    vmem = pl.BlockSpec(memory_space=pltpu.VMEM)
    hbm = pl.BlockSpec(memory_space=pltpu.HBM)
    flat = jax.ShapeDtypeStruct((tok, cols), F32)
    kept = pltpu.VMEM((heads, tok, DH), F32)
    rows_bf = pltpu.VMEM((tok, cols), BF)
    head_bf = pltpu.VMEM((heads, tok, DH), BF)
    mat_bf = pltpu.VMEM((heads, DH, DH), BF)
    mats_bf = pltpu.VMEM((heads, DH, 2 * DH), BF)
    turned_bf = pltpu.VMEM((2, heads, DH, half), BF)
    vec = pltpu.VMEM((heads, DH, half), F32)
    results = pl.pallas_call(
        functools.partial(mega, span, n_seq, n_head),
        name="layer",
        out_shape=[kept, kept, kept, pltpu.VMEM((heads, tok, DH), BF), pltpu.VMEM((heads, 2 * DH, DH), BF)],
        in_specs=[hbm] * 6,
        out_specs=[vmem] * 5,
        scratch_shapes=[
            pltpu.SMEM((heads,), F32), rows_bf, rows_bf, pltpu.VMEM((n_head,) + d_layer.shape, BF),
            pltpu.VMEM(out_weight.shape, BF), pltpu.VMEM((tok, cols), F32), rows_bf, rows_bf, turned_bf,
            mats_bf, mats_bf, pltpu.VMEM((slots, heads, DH, 2 * DH), BF), mat_bf, mat_bf, mat_bf, mat_bf,
            pltpu.VMEM((slots, heads, DH, DH), BF), pltpu.VMEM((slots, heads, DH, DH), BF),
            head_bf, head_bf, turned_bf, turned_bf, turned_bf,
            rows_bf, rows_bf, head_bf, pltpu.VMEM((heads, DH, half), BF),
            pltpu.VMEM((2, heads, tok, 2 * DH), BF),
            pltpu.VMEM((2, heads, DH, tok), BF),
            pltpu.VMEM((2, heads, tok, DH), BF),
            pltpu.VMEM((heads, tok, 2 * DH), BF),
            pltpu.VMEM((2, heads, DH, tok), BF),
            pltpu.VMEM((2, heads, half, tok), BF),
            pltpu.VMEM((2, heads, half, half), F32),
            pltpu.VMEM((2, heads, DH, 2 * DH), F32),
            pltpu.VMEM((2, heads, DH, 2 * DH), BF),
            pltpu.VMEM((2, heads, DH, 2 * DH), BF),
            vec, vec, pltpu.VMEM((heads, 2 * DH, half), BF), vec, vec,
            pltpu.VMEM((heads, 1, half), F32),
            pltpu.SemaphoreType.DMA((6,)),
            pltpu.SemaphoreType.DMA((2 * PIECES * n_head,)),
            pltpu.SemaphoreType.DMA((PIECES * n_head,)),
            pltpu.SemaphoreType.DMA((copies,)),
            pltpu.SemaphoreType.DMA((copies,)),
        ],
        compiler_params=pltpu.CompilerParams(
            collective_id=0, has_side_effects=True, vmem_limit_bytes=48 * 1024 * 1024
        ),
    )(*(
        pltpu.with_memory_space_constraint(array, pltpu.HBM)
        for array in (ridge_scale, key_rows, values, d_layer, out_weight, saved_solutions)
    ))
    return pl.pallas_call(
        store,
        name="store",
        out_shape=[flat, flat, flat],
        in_specs=[vmem] * 5,
        out_specs=[hbm, hbm, hbm],
        scratch_shapes=[pltpu.VMEM((heads, tok, DH), F32), pltpu.SemaphoreType.DMA((3, heads))],
        compiler_params=pltpu.CompilerParams(vmem_limit_bytes=8 * 1024 * 1024),
    )(*(pltpu.with_memory_space_constraint(result, pltpu.VMEM) for result in results))


def solution(mesh):
    return jax.shard_map(
        body,
        mesh=mesh,
        in_specs=(
            P("seq", "head"),
            P("seq", "head"),
            P("seq", "head"),
            P("head", None),
            P("seq", "head"),
            P("head"),
        ),
        out_specs=(P("seq", "head"), P("seq", "head"), P("seq", "head")),
        check_vma=False,
    )
```

```python
import functools
import jax
import jax.numpy as jnp
from jax import lax
from jax.experimental import pallas as pl
from jax.experimental.pallas import tpu as pltpu
from jax.sharding import PartitionSpec as P

DH = 128
ITERS = 8
PIECES = 4
EPSILON = 1e-06
BF = jnp.bfloat16
F32 = jnp.float32
MESH = pl.DeviceIdType.MESH


def nn(left, right):
    return lax.dot_general(left, right, (((1,), (0,)), ((), ())), preferred_element_type=F32)


def nt(left, right):
    return lax.dot_general(left, right, (((1,), (1,)), ((), ())), preferred_element_type=F32)


def split(a):
    hi = a.astype(BF)
    return hi, (a - hi.astype(F32)).astype(BF)


def flip(a):
    return a.astype(F32).T.astype(BF)


def beside(*parts):
    return jnp.concatenate(parts, axis=1)


def above(*parts):
    return jnp.concatenate(parts, axis=0)


def own_mask(tok):
    key_ids = lax.broadcasted_iota(jnp.int32, (tok, tok), 0)
    tok_ids = lax.broadcasted_iota(jnp.int32, (tok, tok), 1)
    return key_ids <= tok_ids


def window_masked(scores):
    tok = scores.shape[1]
    own = own_mask(tok)
    return above(jnp.where(own, scores[:tok], 0.0), jnp.where(own, 0.0, scores[tok:]))


def slots_sum(ref, h):
    total = ref[0, h].astype(F32)
    for slot in range(1, ref.shape[0]):
        total = total + ref[slot, h].astype(F32)
    return total


def mega(span, n_seq, n_head, ridge_hbm, key_hbm, val_hbm, d_hbm, w_hbm, sav_hbm, gq, gk, gv, key_out, sym_out,
         ridge, key, val, d_all, w, sav, key_lag, val_lag, ot_s,
         mid, mid_lag, mid_in, cross, sym, cross_lead, sym_lead, cross_in, sym_in,
         x_bf, x_lead, o_lead, y_bf, y_lead, key_stop, val_stop, x_stop, o_stop, sym_first,
         k2_s, kt_s, vc_s, xs_s, xt_s, a1_s, vs_s, full_s, g_s, st_s, r_s, p_s, p2_s, ya_s, yb_s, rr_s,
         local_sem, dsend_sem, drecv_sem, send_sem, recv_sem):
    s = lax.axis_index("seq")
    me = lax.axis_index("head")
    heads = ridge.shape[0]
    tok = key.shape[0]
    half = tok // 2
    width = d_all.shape[2]
    rows = [slice(0, half), slice(half, tok)]
    pieces = [range(0, PIECES // 2), range(PIECES // 2, PIECES)]
    y_s = [ya_s, yb_s]
    d_copy_in = pltpu.make_async_copy(d_hbm, d_all.at[me], local_sem.at[0])
    key_copy = pltpu.make_async_copy(key_hbm, key, local_sem.at[1])
    val_copy = pltpu.make_async_copy(val_hbm, val, local_sem.at[2])
    w_copy = pltpu.make_async_copy(w_hbm, w, local_sem.at[3])
    x_copy = pltpu.make_async_copy(sav_hbm, sav, local_sem.at[4])
    ridge_copy = pltpu.make_async_copy(ridge_hbm, ridge, local_sem.at[5])
    for copy in (d_copy_in, key_copy, val_copy, x_copy, w_copy, ridge_copy):
        copy.start()

    def exists(d):
        return s + d < n_seq if d > 0 else s + d >= 0

    paired = span == 2
    odd = lax.rem(s, 2) == 1
    even = jnp.logical_not(odd)
    detour = paired and n_seq == 8
    barrier = pltpu.get_barrier_semaphore()
    has_right, has_left = me + 1 < n_head, me > 0
    for there, step in ((has_right, 1), (has_left, -1)):
        @pl.when(there)
        def _():
            pl.semaphore_signal(barrier, inc=1, device_id={"head": me + step}, device_id_type=MESH)
    for d in [d for m in range(1, span + 1) for d in (m, -m)]:
        @pl.when(exists(d))
        def _():
            pl.semaphore_signal(barrier, inc=1, device_id={"seq": s + d}, device_id_type=MESH)
    if detour:
        @pl.when(odd)
        def _():
            far = lax.rem(s + n_seq // 2, n_seq)
            pl.semaphore_signal(barrier, inc=1, device_id={"seq": far}, device_id_type=MESH)
    pl.semaphore_wait(
        barrier,
        (lax.rem(s, 2) if detour else 0) +
        jnp.minimum(me, 1) + jnp.minimum(n_head - 1 - me, 1)
        + jnp.minimum(s, span) + jnp.minimum(n_seq - 1 - s, span),
    )

    counter = [0]
    hops = []

    class Hop:
        def __init__(self, source, target, d, sender=None, receiver=None, skip=None):
            self.sender = exists(d) if sender is None else sender
            self.receiver = exists(-d) if receiver is None else receiver
            if skip is not None:
                self.sender = jnp.logical_and(self.sender, s != skip[0])
                self.receiver = jnp.logical_and(self.receiver, s != skip[1])
            self.copy = pltpu.make_async_remote_copy(
                src_ref=source,
                dst_ref=target,
                send_sem=send_sem.at[counter[0]],
                recv_sem=recv_sem.at[counter[0]],
                device_id={"seq": s + d},
                device_id_type=MESH,
            )
            counter[0] += 1
            hops.append(self)
            if receiver is None:
                @pl.when(jnp.logical_not(exists(-d)))
                def _():
                    target[...] = jnp.zeros(target.shape, target.dtype)

        def start(self):
            pl.when(self.sender)(self.copy.start)
            return self

        def arrive(self):
            pl.when(self.receiver)(self.copy.wait_recv)

        def finish(self):
            pl.when(self.sender)(self.copy.wait_send)

    class Route:
        def __init__(self, source, target, d, stop):
            a, b = n_seq // 2 - d // 2, n_seq // 2 + d // 2
            way = (a + n_seq // 2) % n_seq
            self.direct = Hop(source, target, d, skip=(a, b) if detour else None).start()
            self.legs = []
            if detour:
                self.legs = [
                    Hop(source, stop, way - a, s == a, s == way).start(),
                    Hop(stop, target, b - way, s == way, s == b),
                ]

        def forward(self):
            if self.legs:
                self.legs[0].arrive()
                self.legs[1].start()

        def arrive(self):
            self.direct.arrive()
            if self.legs:
                self.legs[1].arrive()

    def mids(source, target, sign):
        return [Hop(source, target.at[m - 1], sign * m).start() for m in range(1, span)]

    def d_copy(origin, q, step):
        piece = d_all.at[origin, pl.ds(q * (tok // PIECES), tok // PIECES)]
        place = origin * PIECES + q
        return pltpu.make_async_remote_copy(
            src_ref=piece,
            dst_ref=piece,
            send_sem=dsend_sem.at[place + (0 if step > 0 else PIECES * n_head)],
            recv_sem=drecv_sem.at[place],
            device_id={"head": me + step},
            device_id_type=MESH,
        )

    def d_start(q):
        pl.when(has_right)(lambda: d_copy(me, q, 1).start())
        pl.when(has_left)(lambda: d_copy(me, q, -1).start())

    def d_relay(k, q):
        @pl.when(jnp.logical_and(me - k >= 0, has_right))
        def _():
            copy = d_copy(me - k, q, 1)
            copy.wait_recv()
            copy.start()

        @pl.when(jnp.logical_and(me + k < n_head, has_left))
        def _():
            copy = d_copy(me + k, q, -1)
            copy.wait_recv()
            copy.start()

    at_end = jnp.logical_or(me == 0, me == n_head - 1)

    def project(c):
        acc = None
        for i in range(n_head):
            origin = jnp.where(me == 0, i, n_head - 1 - i)
            if i:
                @pl.when(at_end)
                def _():
                    for q in pieces[c]:
                        d_copy(origin, q, 1).wait_recv()
            col = pl.multiple_of(origin * width, width)
            part = nt(w[:, pl.ds(col, width)], d_all[origin, rows[c]])
            acc = part if acc is None else acc + part
        for h in range(heads):
            ot_s[c, h] = acc[h * DH : (h + 1) * DH].astype(BF)

    def cols(h):
        return slice(h * DH, (h + 1) * DH)

    d_copy_in.wait()
    for q in pieces[0]:
        d_start(q)
    key_copy.wait()
    key_hop = Route(key, key_lag, span, key_stop)
    val_copy.wait()
    val_hop = Route(val, val_lag, span, val_stop)
    for h in range(heads):
        total = None
        for c in range(2):
            k, v = key[rows[c], cols(h)], val[rows[c], cols(h)]
            kt = flip(k)
            kt_s[c, h, :, :half] = kt
            k2_s[c, h, :half] = beside(k, k)
            vc_s[c, h, :half] = v
            both = nn(kt, beside(k, v))
            if c == 0:
                full_s[1, h] = both
            total = both if total is None else total + both
        mid[h] = total.astype(BF)
    if paired:
        mid_hops = [Hop(mid, mid_in.at[0], 1, even, odd).start()]
    else:
        mid_hops = mids(mid, mid_in, 1)
    x_copy.wait()
    for h in range(heads):
        x_hi, x_lo = split(sav[:, cols(h)])
        x_bf[h] = x_hi
        xs_s[h] = beside(x_hi, x_lo)
    x_hop = Route(x_bf, x_lead, -span, x_stop)
    for h in range(heads):
        for c in range(2):
            xt_s[c, h] = beside(*split(sav[rows[c], cols(h)].T))
            scores = nt(k2_s[c, h, :half], xs_s[h, rows[c]])
            a1_s[c, h] = beside(*split(jnp.where(own_mask(half), scores, 0.0)))
    late = list(pieces[1])
    for k in range(1, max(n_head - 1, len(late) + 1)):
        if k < n_head - 1:
            for q in pieces[0]:
                d_relay(k, q)
        if late:
            d_start(late.pop(0))
        if k == 1:
            key_hop.forward()
    val_hop.forward()
    x_hop.forward()
    rest = [(k, q) for k in range(1, n_head - 1) for q in pieces[1]]
    for k, q in rest[:2]:
        d_relay(k, q)
    rest = rest[2:]
    for h in range(heads):
        key_out[h] = key[:, cols(h)]
    w_copy.wait()
    ridge_copy.wait()
    project(0)
    o_hops = [Route(ot_s.at[0], o_lead.at[0], -span, o_stop)]
    key_hop.arrive()
    for h in range(heads):
        for c in range(2):
            k = key_lag[rows[c], cols(h)]
            kt_s[c, h, :, half:] = flip(k)
            k2_s[c, h, half:] = beside(k, k)
    val_hop.arrive()
    for h in range(heads):
        for c in range(2):
            vc_s[c, h, half:] = val_lag[rows[c], cols(h)]
        late = nn(kt_s[1, h, :, half:], beside(k2_s[1, h, half:, :DH], vc_s[1, h, half:]))
        full_s[0, h] = late
        if paired:
            early = nn(kt_s[0, h, :, half:], beside(k2_s[0, h, half:, :DH], vc_s[0, h, half:]))
            mid_lag[h] = (early + late).astype(BF)
    if paired:
        mid_hops.append(Hop(mid_lag, mid_in.at[0], -1, odd, even).start())
    for k, q in rest[: len(rest) // 2]:
        d_relay(k, q)
    for hop in mid_hops:
        hop.arrive()
    for h in range(heads):
        for c in range(2):
            total = full_s[c, h]
            if span > 1:
                total = total + slots_sum(mid_in, h)
            g_hi, g_lo = split(total[:, :DH])
            g_s[c, h] = beside(g_hi, g_hi)
            st_s[c, h] = beside(*split(total[:, DH:]))

    def begin(c):
        outs = [ot_s[c, h] for h in range(heads)]
        scores = [nn(vc_s[c, h], outs[h]) for h in range(heads)]
        base = [nn(st_s[c, h], above(outs[h], outs[h])) for h in range(heads)]
        parts = []
        for h in range(heads):
            masked = window_masked(scores[h])
            vs_s[c, h] = masked[:half]
            parts.append(split(masked))
        rs = [base[h] + nn(kt_s[c, h], parts[h][0]) + nn(kt_s[c, h], parts[h][1]) for h in range(heads)]
        for h in range(heads):
            r_s[h] = rs[h]
            p_s[h] = rs[h]
            p2_s[h] = above(*split(rs[h]))
            y_s[c][h] = jnp.zeros_like(rs[h])
            rr_s[h] = jnp.sum(rs[h] * rs[h], axis=0, keepdims=True)

    def iterate(c, between=None):
        def curves():
            smooths, scores = [], []
            for h in range(heads):
                scores.append(nn(k2_s[c, h], p2_s[h]))
                smooths.append(nn(g_s[c, h], p2_s[h]))
            result = []
            for h in range(heads):
                p = p_s[h]
                masked = window_masked(scores[h])
                smooth = smooths[h] + ridge[h] * p
                curve = jnp.sum(masked * masked, axis=0, keepdims=True)
                curve = curve + jnp.sum(p * smooth, axis=0, keepdims=True)
                result.append((masked, smooth, curve + EPSILON))
            return result

        def step(i, carry):
            found = curves()
            images = [nn(kt_s[c, h], found[h][0].astype(BF)) + found[h][1] for h in range(heads)]
            for h in range(heads):
                p = p_s[h]
                rr = rr_s[h]
                alpha = rr / found[h][2]
                y_s[c][h] = y_s[c][h] + alpha * p
                r = r_s[h] - alpha * images[h]
                r_s[h] = r
                nr = jnp.sum(r * r, axis=0, keepdims=True)
                p = r + nr / (rr + EPSILON) * p
                p_s[h] = p
                p2_s[h] = above(*split(p))
                rr_s[h] = nr
            return carry

        if between is None:
            lax.fori_loop(0, ITERS - 1, step, 0)
        else:
            lax.fori_loop(0, 1, step, 0)
            between()
            lax.fori_loop(1, ITERS - 1, step, 0)
        found = curves()
        for h in range(heads):
            y = y_s[c][h] + rr_s[h] / found[h][2] * p_s[h]
            y_s[c][h] = y
            y_bf[c, h] = y.astype(BF)

    every = list(range(heads))

    def twice(a):
        return beside(a, a)

    def negative_sym(pair):
        return -(pair + pair.T)

    def apply_states(c_f, s_f, k, v):
        c_hi, c_lo = split(c_f)
        to_k = nt(twice(v), beside(c_hi, c_lo))
        if s_f is not None:
            to_k = to_k + nn(twice(k), above(*split(s_f)))
        return to_k, nn(twice(k), above(c_hi, c_lo))

    def apply_cross():
        for h in every:
            to_k, to_v = apply_states(slots_sum(cross_in, h), None, key[:, cols(h)], val[:, cols(h)])
            gk[h] = gk[h] + to_k
            gv[h] = gv[h] + to_v

    def halfway():
        for k, q in rest[len(rest) // 2 :]:
            d_relay(k, q)

    begin(0)
    iterate(0, halfway)
    y_hops = [Hop(y_bf.at[0], y_lead.at[0], -span).start()]
    o_hops[0].forward()
    project(1)
    o_hops.append(Hop(ot_s.at[1], o_lead.at[1], -span).start())
    begin(1)
    iterate(1)
    y_hops.append(Hop(y_bf.at[1], y_lead.at[1], -span).start())

    crosses = [[nt(xt_s[c, h], twice(ot_s[c, h])) for h in every] for c in range(2)]
    pairs = [[], []]
    for c in range(2):
        for h in every:
            y_hi, y_lo = split(y_s[c][h])
            pairs[c].append(nt(xt_s[c, h], twice(y_hi)) + nt(xt_s[c, h, :, :half], y_lo))
    for h in every:
        cross[h] = (crosses[0][h] + crosses[1][h]).astype(BF)
        sym[h] = negative_sym(pairs[0][h] + pairs[1][h]).astype(BF)
    if paired:
        cross_hops = [Hop(cross, cross_in.at[0], -1, odd, even).start()]
        sym_hops = [Hop(sym, sym_in.at[0], -1, odd, even).start()]
    else:
        cross_hops, sym_hops = mids(cross, cross_in, -1), mids(sym, sym_in, -1)
    for h in every:
        to_k, to_v = apply_states(
            crosses[1][h], negative_sym(pairs[1][h]), k2_s[0, h, :half, :DH], vc_s[0, h, :half]
        )
        gk[h, rows[0]] = to_k
        gv[h, rows[0]] = to_v + nt(a1_s[0, h], twice(ot_s[0, h]))
        gv[h, rows[1]] = nt(a1_s[1, h], twice(ot_s[1, h]))
    own = own_mask(half)
    for c in range(2):
        ys = [split(y_s[c][h]) for h in every]
        scores = [nn(k2_s[c, h, :half], above(*ys[h])) for h in every]
        for h in every:
            y_hi, y_lo = ys[h]
            a2_hi, a2_lo = split(vs_s[c, h] - jnp.where(own, scores[h], 0.0))
            x_hi, x_lo = xs_s[h, rows[c], :DH], xs_s[h, rows[c], DH:]
            a1 = a1_s[c, h]
            g = nn(beside(a2_hi, a2_lo), above(x_hi, x_hi)) + nn(a2_hi, x_lo)
            g = g - nt(a1, twice(y_hi)) - nt(a1[:, :half], y_lo)
            gk[h, rows[c]] = gk[h, rows[c]] + g if c == 0 else g
    for h in every:
        for c in range(2):
            gq[h, rows[c]] = y_s[c][h].T

    x_hop.arrive()
    for hop in o_hops:
        hop.arrive()
    seen = []
    for c in range(2):
        scores = [nt(k2_s[c, h, :half, :DH], x_lead[h, rows[c]]) for h in every]
        seen.append([beside(*split(jnp.where(own, 0.0, t))) for t in scores])
        for h in every:
            gv[h, rows[c]] = gv[h, rows[c]] + nt(seen[c][h], twice(o_lead[c, h]))
    flipped = [[flip(x_lead[h, rows[c]]) for h in every] for c in range(2)]
    crosses = [[nt(flipped[c][h], o_lead[c, h]) for h in every] for c in range(2)]
    if paired:
        for h in every:
            cross_lead[h] = (crosses[0][h] + crosses[1][h]).astype(BF)
        cross_hops.append(Hop(cross_lead, cross_in.at[0], 1, even, odd).start())

    def lead_part(c):
        scores = []
        for h in every:
            vk = beside(vc_s[c, h, :half], k2_s[c, h, :half, :DH])
            scores.append(nn(vk, above(o_lead[c, h], -y_lead[c, h])))
        for h in every:
            a2_hi, a2_lo = split(jnp.where(own, 0.0, scores[h]))
            x = x_lead[h, rows[c]]
            g = nn(beside(a2_hi, a2_lo), above(x, x)) - nt(seen[c][h], twice(y_lead[c, h]))
            gk[h, rows[c]] = gk[h, rows[c]] + g

    y_hops[0].arrive()
    pairs = [nt(flipped[0][h], y_lead[0, h]) for h in every]
    for h in every:
        state = negative_sym(pairs[h])
        sym_first[h] = state
        to_k, to_v = apply_states(crosses[0][h], state, k2_s[1, h, :half, :DH], vc_s[1, h, :half])
        gk[h, rows[1]] = gk[h, rows[1]] + to_k
        gv[h, rows[1]] = gv[h, rows[1]] + to_v
    lead_part(0)
    for hop in cross_hops:
        hop.arrive()
    if span > 1:
        apply_cross()
    y_hops[1].arrive()
    if paired:
        lates = [nt(flipped[1][h], y_lead[1, h]) + nt(y_lead[1, h], flipped[1][h]) for h in every]
        for h in every:
            sym_lead[h] = (sym_first[h] - lates[h]).astype(BF)
        sym_hops.append(Hop(sym_lead, sym_in.at[0], 1, even, odd).start())
    lead_part(1)
    for hop in sym_hops:
        hop.arrive()
    for h in every:
        sym_out[h] = above(*split(slots_sum(sym_in, h))) if span > 1 else jnp.zeros(sym_out.shape[1:], BF)
    for j in range(n_head):
        @pl.when(jnp.logical_and(has_right, j <= me))
        def _():
            for q in range(PIECES):
                d_copy(j, q, 1).wait_send()

        @pl.when(jnp.logical_and(has_left, j >= me))
        def _():
            for q in range(PIECES):
                d_copy(j, q, -1).wait_send()
    for hop in hops:
        hop.finish()


def store(gq, gk, gv, key, sym, gq_hbm, gk_hbm, gv_hbm, total, sem):
    heads = gk.shape[0]

    def copies(i, source, target):
        return [
            pltpu.make_async_copy(source.at[h], target.at[:, pl.ds(h * DH, DH)], sem.at[i, h])
            for h in range(heads)
        ]

    early = copies(0, gq, gq_hbm) + copies(1, gv, gv_hbm)
    late = copies(2, total, gk_hbm)
    for copy in early:
        copy.start()
    for h in range(heads):
        k = key[h]
        total[h] = gk[h] + nn(beside(k, k), sym[h])
        late[h].start()
    for copy in early + late:
        copy.wait()


def body(key_rows, values, d_layer, out_weight, saved_solutions, ridge_scale):
    tok, cols = key_rows.shape
    heads = cols // DH
    half = tok // 2
    n_seq, n_head = lax.axis_size("seq"), lax.axis_size("head")
    span = n_seq // 4
    slots = max(span - 1, 1)
    copies = 15 + (6 if span == 2 else 3 * (span - 1))
    vmem = pl.BlockSpec(memory_space=pltpu.VMEM)
    hbm = pl.BlockSpec(memory_space=pltpu.HBM)
    flat = jax.ShapeDtypeStruct((tok, cols), F32)
    kept = pltpu.VMEM((heads, tok, DH), F32)
    rows_bf = pltpu.VMEM((tok, cols), BF)
    head_bf = pltpu.VMEM((heads, tok, DH), BF)
    mat_bf = pltpu.VMEM((heads, DH, DH), BF)
    mats_bf = pltpu.VMEM((heads, DH, 2 * DH), BF)
    turned_bf = pltpu.VMEM((2, heads, DH, half), BF)
    vec = pltpu.VMEM((heads, DH, half), F32)
    results = pl.pallas_call(
        functools.partial(mega, span, n_seq, n_head),
        name="layer",
        out_shape=[kept, kept, kept, pltpu.VMEM((heads, tok, DH), BF), pltpu.VMEM((heads, 2 * DH, DH), BF)],
        in_specs=[hbm] * 6,
        out_specs=[vmem] * 5,
        scratch_shapes=[
            pltpu.SMEM((heads,), F32), rows_bf, rows_bf, pltpu.VMEM((n_head,) + d_layer.shape, BF),
            pltpu.VMEM(out_weight.shape, BF), pltpu.VMEM((tok, cols), F32), rows_bf, rows_bf, turned_bf,
            mats_bf, mats_bf, pltpu.VMEM((slots, heads, DH, 2 * DH), BF), mat_bf, mat_bf, mat_bf, mat_bf,
            pltpu.VMEM((slots, heads, DH, DH), BF), pltpu.VMEM((slots, heads, DH, DH), BF),
            head_bf, head_bf, turned_bf, turned_bf, turned_bf,
            rows_bf, rows_bf, head_bf, pltpu.VMEM((heads, DH, half), BF), pltpu.VMEM((heads, DH, DH), F32),
            pltpu.VMEM((2, heads, tok, 2 * DH), BF),
            pltpu.VMEM((2, heads, DH, tok), BF),
            pltpu.VMEM((2, heads, tok, DH), BF),
            pltpu.VMEM((heads, tok, 2 * DH), BF),
            pltpu.VMEM((2, heads, DH, tok), BF),
            pltpu.VMEM((2, heads, half, tok), BF),
            pltpu.VMEM((2, heads, half, half), F32),
            pltpu.VMEM((2, heads, DH, 2 * DH), F32),
            pltpu.VMEM((2, heads, DH, 2 * DH), BF),
            pltpu.VMEM((2, heads, DH, 2 * DH), BF),
            vec, vec, pltpu.VMEM((heads, 2 * DH, half), BF), vec, vec,
            pltpu.VMEM((heads, 1, half), F32),
            pltpu.SemaphoreType.DMA((6,)),
            pltpu.SemaphoreType.DMA((2 * PIECES * n_head,)),
            pltpu.SemaphoreType.DMA((PIECES * n_head,)),
            pltpu.SemaphoreType.DMA((copies,)),
            pltpu.SemaphoreType.DMA((copies,)),
        ],
        compiler_params=pltpu.CompilerParams(
            collective_id=0, has_side_effects=True, vmem_limit_bytes=48 * 1024 * 1024
        ),
    )(*(
        pltpu.with_memory_space_constraint(array, pltpu.HBM)
        for array in (ridge_scale, key_rows, values, d_layer, out_weight, saved_solutions)
    ))
    return pl.pallas_call(
        store,
        name="store",
        out_shape=[flat, flat, flat],
        in_specs=[vmem] * 5,
        out_specs=[hbm, hbm, hbm],
        scratch_shapes=[pltpu.VMEM((heads, tok, DH), F32), pltpu.SemaphoreType.DMA((3, heads))],
        compiler_params=pltpu.CompilerParams(vmem_limit_bytes=8 * 1024 * 1024),
    )(*(pltpu.with_memory_space_constraint(result, pltpu.VMEM) for result in results))


def solution(mesh):
    return jax.shard_map(
        body,
        mesh=mesh,
        in_specs=(
            P("seq", "head"),
            P("seq", "head"),
            P("seq", "head"),
            P("head", None),
            P("seq", "head"),
            P("head"),
        ),
        out_specs=(P("seq", "head"), P("seq", "head"), P("seq", "head")),
        check_vma=False,
    )
```

```python
import functools
import jax
import jax.numpy as jnp
from jax import lax
from jax.experimental import pallas as pl
from jax.experimental.pallas import tpu as pltpu
from jax.sharding import PartitionSpec as P

DH = 128
ITERS = 8
PIECES = 4
EPSILON = 1e-06
BF = jnp.bfloat16
F32 = jnp.float32
MESH = pl.DeviceIdType.MESH


def nn(left, right):
    return lax.dot_general(left, right, (((1,), (0,)), ((), ())), preferred_element_type=F32)


def nt(left, right):
    return lax.dot_general(left, right, (((1,), (1,)), ((), ())), preferred_element_type=F32)


def split(a):
    hi = a.astype(BF)
    return hi, (a - hi.astype(F32)).astype(BF)


def flip(a):
    return a.astype(F32).T.astype(BF)


def beside(*parts):
    return jnp.concatenate(parts, axis=1)


def above(*parts):
    return jnp.concatenate(parts, axis=0)


def own_mask(tok):
    key_ids = lax.broadcasted_iota(jnp.int32, (tok, tok), 0)
    tok_ids = lax.broadcasted_iota(jnp.int32, (tok, tok), 1)
    return key_ids <= tok_ids


def window_masked(scores):
    tok = scores.shape[1]
    own = own_mask(tok)
    return above(jnp.where(own, scores[:tok], 0.0), jnp.where(own, 0.0, scores[tok:]))


def slots_sum(ref, h):
    total = ref[0, h].astype(F32)
    for slot in range(1, ref.shape[0]):
        total = total + ref[slot, h].astype(F32)
    return total


def mega(span, n_seq, n_head, ridge_hbm, key_hbm, val_hbm, d_hbm, w_hbm, sav_hbm, gq, gk, gv, key_out, sym_out,
         ridge, key, val, d_all, w, sav, key_lag, val_lag, ot_s,
         mid, mid_lag, mid_in, cross, sym, cross_lead, sym_lead, cross_in, sym_in,
         x_bf, x_lead, o_lead, y_bf, y_lead, key_stop, val_stop, x_stop, o_stop, sym_first,
         k2_s, kt_s, vc_s, xs_s, xt_s, a1_s, vs_s, full_s, g_s, st_s, r_s, p_s, p2_s, ya_s, yb_s, rr_s,
         local_sem, dsend_sem, drecv_sem, send_sem, recv_sem):
    s = lax.axis_index("seq")
    me = lax.axis_index("head")
    heads = ridge.shape[0]
    tok = key.shape[0]
    half = tok // 2
    width = d_all.shape[2]
    rows = [slice(0, half), slice(half, tok)]
    pieces = [range(0, PIECES // 2), range(PIECES // 2, PIECES)]
    y_s = [ya_s, yb_s]
    d_copy_in = pltpu.make_async_copy(d_hbm, d_all.at[me], local_sem.at[0])
    key_copy = pltpu.make_async_copy(key_hbm, key, local_sem.at[1])
    val_copy = pltpu.make_async_copy(val_hbm, val, local_sem.at[2])
    w_copy = pltpu.make_async_copy(w_hbm, w, local_sem.at[3])
    x_copy = pltpu.make_async_copy(sav_hbm, sav, local_sem.at[4])
    ridge_copy = pltpu.make_async_copy(ridge_hbm, ridge, local_sem.at[5])
    for copy in (d_copy_in, key_copy, val_copy, x_copy, w_copy, ridge_copy):
        copy.start()

    def exists(d):
        return s + d < n_seq if d > 0 else s + d >= 0

    paired = span == 2
    odd = lax.rem(s, 2) == 1
    even = jnp.logical_not(odd)
    detour = paired and n_seq == 8
    barrier = pltpu.get_barrier_semaphore()
    has_right, has_left = me + 1 < n_head, me > 0
    for there, step in ((has_right, 1), (has_left, -1)):
        @pl.when(there)
        def _():
            pl.semaphore_signal(barrier, inc=1, device_id={"head": me + step}, device_id_type=MESH)
    for d in [d for m in range(1, span + 1) for d in (m, -m)]:
        @pl.when(exists(d))
        def _():
            pl.semaphore_signal(barrier, inc=1, device_id={"seq": s + d}, device_id_type=MESH)
    if detour:
        @pl.when(odd)
        def _():
            far = lax.rem(s + n_seq // 2, n_seq)
            pl.semaphore_signal(barrier, inc=1, device_id={"seq": far}, device_id_type=MESH)
    pl.semaphore_wait(
        barrier,
        (lax.rem(s, 2) if detour else 0) +
        jnp.minimum(me, 1) + jnp.minimum(n_head - 1 - me, 1)
        + jnp.minimum(s, span) + jnp.minimum(n_seq - 1 - s, span),
    )

    counter = [0]
    hops = []

    class Hop:
        def __init__(self, source, target, d, sender=None, receiver=None, skip=None):
            self.sender = exists(d) if sender is None else sender
            self.receiver = exists(-d) if receiver is None else receiver
            if skip is not None:
                self.sender = jnp.logical_and(self.sender, s != skip[0])
                self.receiver = jnp.logical_and(self.receiver, s != skip[1])
            self.copy = pltpu.make_async_remote_copy(
                src_ref=source,
                dst_ref=target,
                send_sem=send_sem.at[counter[0]],
                recv_sem=recv_sem.at[counter[0]],
                device_id={"seq": s + d},
                device_id_type=MESH,
            )
            counter[0] += 1
            hops.append(self)
            if receiver is None:
                @pl.when(jnp.logical_not(exists(-d)))
                def _():
                    target[...] = jnp.zeros(target.shape, target.dtype)

        def start(self, only=None):
            pl.when(self.sender if only is None else jnp.logical_and(self.sender, only))(self.copy.start)
            return self

        def arrive(self):
            pl.when(self.receiver)(self.copy.wait_recv)

        def finish(self):
            pl.when(self.sender)(self.copy.wait_send)

    class Route:
        def __init__(self, source, target, d, stop):
            a, b = n_seq // 2 - d // 2, n_seq // 2 + d // 2
            way = (a + n_seq // 2) % n_seq
            self.direct = Hop(source, target, d, skip=(a, b) if detour else None).start()
            self.legs = []
            if detour:
                self.legs = [
                    Hop(source, stop, way - a, s == a, s == way).start(),
                    Hop(stop, target, b - way, s == way, s == b),
                ]

        def forward(self):
            if self.legs:
                self.legs[0].arrive()
                self.legs[1].start()

        def arrive(self):
            self.direct.arrive()
            if self.legs:
                self.legs[1].arrive()

    def mids(source, target, sign):
        return [Hop(source, target.at[m - 1], sign * m).start() for m in range(1, span)]

    def d_copy(origin, q, step):
        piece = d_all.at[origin, pl.ds(q * (tok // PIECES), tok // PIECES)]
        place = origin * PIECES + q
        return pltpu.make_async_remote_copy(
            src_ref=piece,
            dst_ref=piece,
            send_sem=dsend_sem.at[place + (0 if step > 0 else PIECES * n_head)],
            recv_sem=drecv_sem.at[place],
            device_id={"head": me + step},
            device_id_type=MESH,
        )

    def d_start(q, only=True):
        pl.when(jnp.logical_and(has_right, only))(lambda: d_copy(me, q, 1).start())
        pl.when(jnp.logical_and(has_left, only))(lambda: d_copy(me, q, -1).start())

    def d_relay(k, q):
        @pl.when(jnp.logical_and(me - k >= 0, has_right))
        def _():
            copy = d_copy(me - k, q, 1)
            copy.wait_recv()
            copy.start()

        @pl.when(jnp.logical_and(me + k < n_head, has_left))
        def _():
            copy = d_copy(me + k, q, -1)
            copy.wait_recv()
            copy.start()

    at_end = jnp.logical_or(me == 0, me == n_head - 1)

    def project(c):
        acc = None
        for i in range(n_head):
            origin = jnp.where(me == 0, i, n_head - 1 - i)
            if i:
                @pl.when(at_end)
                def _():
                    for q in pieces[c]:
                        d_copy(origin, q, 1).wait_recv()
            col = pl.multiple_of(origin * width, width)
            part = nt(w[:, pl.ds(col, width)], d_all[origin, rows[c]])
            acc = part if acc is None else acc + part
        for h in range(heads):
            ot_s[c, h] = acc[h * DH : (h + 1) * DH].astype(BF)

    def cols(h):
        return slice(h * DH, (h + 1) * DH)

    d_copy_in.wait()
    for q in pieces[0]:
        d_start(q)
    key_copy.wait()
    key_hop = Route(key, key_lag, span, key_stop)
    val_copy.wait()
    val_hop = Route(val, val_lag, span, val_stop)
    for h in range(heads):
        total = None
        for c in range(2):
            k, v = key[rows[c], cols(h)], val[rows[c], cols(h)]
            kt = flip(k)
            kt_s[c, h, :, :half] = kt
            k2_s[c, h, :half] = beside(k, k)
            vc_s[c, h, :half] = v
            both = nn(kt, beside(k, v))
            if c == 0:
                full_s[1, h] = both
            total = both if total is None else total + both
        mid[h] = total.astype(BF)
    if paired:
        mid_hops = [Hop(mid, mid_in.at[0], 1, even, odd).start()]
    else:
        mid_hops = mids(mid, mid_in, 1)
    x_copy.wait()
    for h in range(heads):
        x_hi, x_lo = split(sav[:, cols(h)])
        x_bf[h] = x_hi
        xs_s[h] = beside(x_hi, x_lo)
    x_hop = Route(x_bf, x_lead, -span, x_stop)
    for h in range(heads):
        for c in range(2):
            xt_s[c, h] = beside(*split(sav[rows[c], cols(h)].T))
            scores = nt(k2_s[c, h, :half], xs_s[h, rows[c]])
            a1_s[c, h] = beside(*split(jnp.where(own_mask(half), scores, 0.0)))
    late = list(pieces[1])
    for k in range(1, max(n_head - 1, len(late) + 1)):
        if k < n_head - 1:
            for q in pieces[0]:
                d_relay(k, q)
        if late:
            d_start(late.pop(0), even)
        if k == 1:
            key_hop.forward()
    for q in pieces[1]:
        d_start(q, odd)
    val_hop.forward()
    x_hop.forward()
    rest = [(k, q) for k in range(1, n_head - 1) for q in pieces[1]]
    for k, q in rest[:2]:
        d_relay(k, q)
    rest = rest[2:]
    for h in range(heads):
        key_out[h] = key[:, cols(h)]
    for c in range(2):
        y_s[c][...] = jnp.zeros(y_s[c].shape, F32)
    w_copy.wait()
    ridge_copy.wait()
    project(0)
    o_hops = [Route(ot_s.at[0], o_lead.at[0], -span, o_stop)]
    key_hop.arrive()
    for h in range(heads):
        for c in range(2):
            k = key_lag[rows[c], cols(h)]
            kt_s[c, h, :, half:] = flip(k)
            k2_s[c, h, half:] = beside(k, k)
    val_hop.arrive()
    for h in range(heads):
        for c in range(2):
            vc_s[c, h, half:] = val_lag[rows[c], cols(h)]
        late = nn(kt_s[1, h, :, half:], beside(k2_s[1, h, half:, :DH], vc_s[1, h, half:]))
        full_s[0, h] = late
        if paired:
            early = nn(kt_s[0, h, :, half:], beside(k2_s[0, h, half:, :DH], vc_s[0, h, half:]))
            mid_lag[h] = (early + late).astype(BF)
    if paired:
        mid_hops.append(Hop(mid_lag, mid_in.at[0], -1, odd, even).start())
    for k, q in rest[: len(rest) // 2]:
        d_relay(k, q)
    for hop in mid_hops:
        hop.arrive()
    for h in range(heads):
        for c in range(2):
            total = full_s[c, h]
            if span > 1:
                total = total + slots_sum(mid_in, h)
            g_hi, g_lo = split(total[:, :DH])
            g_s[c, h] = beside(g_hi, g_hi)
            st_s[c, h] = beside(*split(total[:, DH:]))

    def begin(c):
        outs = [ot_s[c, h] for h in range(heads)]
        scores = [nn(vc_s[c, h], outs[h]) for h in range(heads)]
        base = [nn(st_s[c, h], above(outs[h], outs[h])) for h in range(heads)]
        parts = []
        for h in range(heads):
            masked = window_masked(scores[h])
            vs_s[c, h] = masked[:half]
            parts.append(split(masked))
        rs = [base[h] + nn(kt_s[c, h], parts[h][0]) + nn(kt_s[c, h], parts[h][1]) for h in range(heads)]
        for h in range(heads):
            r_s[h] = rs[h]
            p_s[h] = rs[h]
            p2_s[h] = above(*split(rs[h]))
            rr_s[h] = jnp.sum(rs[h] * rs[h], axis=0, keepdims=True)

    def iterate(c, between=None):
        def curves():
            smooths, scores = [], []
            for h in range(heads):
                scores.append(nn(k2_s[c, h], p2_s[h]))
                smooths.append(nn(g_s[c, h], p2_s[h]))
            result = []
            for h in range(heads):
                p = p_s[h]
                masked = window_masked(scores[h])
                smooth = smooths[h] + ridge[h] * p
                curve = jnp.sum(masked * masked, axis=0, keepdims=True)
                curve = curve + jnp.sum(p * smooth, axis=0, keepdims=True)
                result.append((masked, smooth, curve + EPSILON))
            return result

        def step(i, carry):
            found = curves()
            images = [nn(kt_s[c, h], found[h][0].astype(BF)) + found[h][1] for h in range(heads)]
            for h in range(heads):
                p = p_s[h]
                rr = rr_s[h]
                alpha = rr / found[h][2]
                y_s[c][h] = y_s[c][h] + alpha * p
                r = r_s[h] - alpha * images[h]
                r_s[h] = r
                nr = jnp.sum(r * r, axis=0, keepdims=True)
                p = r + nr / (rr + EPSILON) * p
                p_s[h] = p
                p2_s[h] = above(*split(p))
                rr_s[h] = nr
            return carry

        if between is None:
            lax.fori_loop(0, ITERS - 1, step, 0, unroll=True)
        else:
            lax.fori_loop(0, 1, step, 0)
            between()
            lax.fori_loop(1, ITERS - 1, step, 0)
        found = curves()
        for h in range(heads):
            y = y_s[c][h] + rr_s[h] / found[h][2] * p_s[h]
            y_s[c][h] = y
            y_bf[c, h] = y.astype(BF)

    every = list(range(heads))

    def twice(a):
        return beside(a, a)

    def negative_sym(pair):
        return -(pair + pair.T)

    def apply_states(c_f, s_f, k, v):
        c_hi, c_lo = split(c_f)
        to_k = nt(twice(v), beside(c_hi, c_lo))
        if s_f is not None:
            to_k = to_k + nn(twice(k), above(*split(s_f)))
        return to_k, nn(twice(k), above(c_hi, c_lo))

    def apply_cross():
        for h in every:
            to_k, to_v = apply_states(slots_sum(cross_in, h), None, key[:, cols(h)], val[:, cols(h)])
            gk[h] = gk[h] + to_k
            gv[h] = gv[h] + to_v

    def halfway():
        for k, q in rest[len(rest) // 2 :]:
            d_relay(k, q)

    begin(0)
    iterate(0, halfway)
    y_hops = [Hop(y_bf.at[0], y_lead.at[0], -span).start()]
    o_hops[0].forward()
    project(1)
    o_hops.append(Hop(ot_s.at[1], o_lead.at[1], -span).start())
    begin(1)
    iterate(1)
    y_hops.append(Hop(y_bf.at[1], y_lead.at[1], -span).start(even if paired else None))

    crosses = [[nt(xt_s[c, h], twice(ot_s[c, h])) for h in every] for c in range(2)]
    pairs = [[], []]
    for c in range(2):
        for h in every:
            y_hi, y_lo = split(y_s[c][h])
            pairs[c].append(nt(xt_s[c, h], twice(y_hi)) + nt(xt_s[c, h, :, :half], y_lo))
    for h in every:
        cross[h] = (crosses[0][h] + crosses[1][h]).astype(BF)
        sym[h] = negative_sym(pairs[0][h] + pairs[1][h]).astype(BF)
    if paired:
        y_hops[1].start(odd)
        cross_hops = [Hop(cross, cross_in.at[0], -1, odd, even).start()]
        sym_hops = [Hop(sym, sym_in.at[0], -1, odd, even).start()]
    else:
        cross_hops, sym_hops = mids(cross, cross_in, -1), mids(sym, sym_in, -1)
    for h in every:
        to_k, to_v = apply_states(
            crosses[1][h], negative_sym(pairs[1][h]), k2_s[0, h, :half, :DH], vc_s[0, h, :half]
        )
        gk[h, rows[0]] = to_k
        gv[h, rows[0]] = to_v + nt(a1_s[0, h], twice(ot_s[0, h]))
        gv[h, rows[1]] = nt(a1_s[1, h], twice(ot_s[1, h]))
    own = own_mask(half)
    for c in range(2):
        ys = [split(y_s[c][h]) for h in every]
        scores = [nn(k2_s[c, h, :half], above(*ys[h])) for h in every]
        for h in every:
            y_hi, y_lo = ys[h]
            a2_hi, a2_lo = split(vs_s[c, h] - jnp.where(own, scores[h], 0.0))
            x_hi, x_lo = xs_s[h, rows[c], :DH], xs_s[h, rows[c], DH:]
            a1 = a1_s[c, h]
            g = nn(beside(a2_hi, a2_lo), above(x_hi, x_hi)) + nn(a2_hi, x_lo)
            g = g - nt(a1, twice(y_hi)) - nt(a1[:, :half], y_lo)
            gk[h, rows[c]] = gk[h, rows[c]] + g if c == 0 else g
    for h in every:
        for c in range(2):
            gq[h, rows[c]] = y_s[c][h].T

    x_hop.arrive()
    for hop in o_hops:
        hop.arrive()
    seen = []
    for c in range(2):
        scores = [nt(k2_s[c, h, :half, :DH], x_lead[h, rows[c]]) for h in every]
        seen.append([beside(*split(jnp.where(own, 0.0, t))) for t in scores])
        for h in every:
            gv[h, rows[c]] = gv[h, rows[c]] + nt(seen[c][h], twice(o_lead[c, h]))
    flipped = [[flip(x_lead[h, rows[c]]) for h in every] for c in range(2)]
    crosses = [[nt(flipped[c][h], o_lead[c, h]) for h in every] for c in range(2)]
    if paired:
        for h in every:
            cross_lead[h] = (crosses[0][h] + crosses[1][h]).astype(BF)
        cross_hops.append(Hop(cross_lead, cross_in.at[0], 1, even, odd).start())

    def lead_part(c):
        scores = []
        for h in every:
            vk = beside(vc_s[c, h, :half], k2_s[c, h, :half, :DH])
            scores.append(nn(vk, above(o_lead[c, h], -y_lead[c, h])))
        for h in every:
            a2_hi, a2_lo = split(jnp.where(own, 0.0, scores[h]))
            x = x_lead[h, rows[c]]
            g = nn(beside(a2_hi, a2_lo), above(x, x)) - nt(seen[c][h], twice(y_lead[c, h]))
            gk[h, rows[c]] = gk[h, rows[c]] + g

    y_hops[0].arrive()
    pairs = [nt(flipped[0][h], y_lead[0, h]) for h in every]
    for h in every:
        state = negative_sym(pairs[h])
        sym_first[h] = state
        to_k, to_v = apply_states(crosses[0][h], state, k2_s[1, h, :half, :DH], vc_s[1, h, :half])
        gk[h, rows[1]] = gk[h, rows[1]] + to_k
        gv[h, rows[1]] = gv[h, rows[1]] + to_v
    lead_part(0)
    for hop in cross_hops:
        hop.arrive()
    if span > 1:
        apply_cross()
    for j in range(n_head):
        @pl.when(jnp.logical_and(has_right, j <= me))
        def _():
            for q in range(PIECES):
                d_copy(j, q, 1).wait_send()

        @pl.when(jnp.logical_and(has_left, j >= me))
        def _():
            for q in range(PIECES):
                d_copy(j, q, -1).wait_send()
    finished = [hop for hop in hops if hop is not y_hops[1]]
    for hop in finished:
        hop.finish()
    y_hops[1].arrive()
    if paired:
        lates = [nt(flipped[1][h], y_lead[1, h]) + nt(y_lead[1, h], flipped[1][h]) for h in every]
        for h in every:
            sym_lead[h] = (sym_first[h] - lates[h]).astype(BF)
        sym_hops.append(Hop(sym_lead, sym_in.at[0], 1, even, odd).start())
    lead_part(1)
    for hop in sym_hops:
        hop.arrive()
    for h in every:
        sym_out[h] = above(*split(slots_sum(sym_in, h))) if span > 1 else jnp.zeros(sym_out.shape[1:], BF)
    for hop in hops:
        if hop not in finished:
            hop.finish()


def store(gq, gk, gv, key, sym, gq_hbm, gk_hbm, gv_hbm, total, sem):
    heads = gk.shape[0]

    def copies(i, source, target):
        return [
            pltpu.make_async_copy(source.at[h], target.at[:, pl.ds(h * DH, DH)], sem.at[i, h])
            for h in range(heads)
        ]

    early = copies(0, gq, gq_hbm) + copies(1, gv, gv_hbm)
    late = copies(2, total, gk_hbm)
    for copy in early:
        copy.start()
    for h in range(heads):
        k = key[h]
        total[h] = gk[h] + nn(beside(k, k), sym[h])
        late[h].start()
    for copy in early + late:
        copy.wait()


def body(key_rows, values, d_layer, out_weight, saved_solutions, ridge_scale):
    tok, cols = key_rows.shape
    heads = cols // DH
    half = tok // 2
    n_seq, n_head = lax.axis_size("seq"), lax.axis_size("head")
    span = n_seq // 4
    slots = max(span - 1, 1)
    copies = 15 + (6 if span == 2 else 3 * (span - 1))
    vmem = pl.BlockSpec(memory_space=pltpu.VMEM)
    hbm = pl.BlockSpec(memory_space=pltpu.HBM)
    flat = jax.ShapeDtypeStruct((tok, cols), F32)
    kept = pltpu.VMEM((heads, tok, DH), F32)
    rows_bf = pltpu.VMEM((tok, cols), BF)
    head_bf = pltpu.VMEM((heads, tok, DH), BF)
    mat_bf = pltpu.VMEM((heads, DH, DH), BF)
    mats_bf = pltpu.VMEM((heads, DH, 2 * DH), BF)
    turned_bf = pltpu.VMEM((2, heads, DH, half), BF)
    vec = pltpu.VMEM((heads, DH, half), F32)
    results = pl.pallas_call(
        functools.partial(mega, span, n_seq, n_head),
        name="layer",
        out_shape=[kept, kept, kept, pltpu.VMEM((heads, tok, DH), BF), pltpu.VMEM((heads, 2 * DH, DH), BF)],
        in_specs=[hbm] * 6,
        out_specs=[vmem] * 5,
        scratch_shapes=[
            pltpu.SMEM((heads,), F32), rows_bf, rows_bf, pltpu.VMEM((n_head,) + d_layer.shape, BF),
            pltpu.VMEM(out_weight.shape, BF), pltpu.VMEM((tok, cols), F32), rows_bf, rows_bf, turned_bf,
            mats_bf, mats_bf, pltpu.VMEM((slots, heads, DH, 2 * DH), BF), mat_bf, mat_bf, mat_bf, mat_bf,
            pltpu.VMEM((slots, heads, DH, DH), BF), pltpu.VMEM((slots, heads, DH, DH), BF),
            head_bf, head_bf, turned_bf, turned_bf, turned_bf,
            rows_bf, rows_bf, head_bf, pltpu.VMEM((heads, DH, half), BF), pltpu.VMEM((heads, DH, DH), F32),
            pltpu.VMEM((2, heads, tok, 2 * DH), BF),
            pltpu.VMEM((2, heads, DH, tok), BF),
            pltpu.VMEM((2, heads, tok, DH), BF),
            pltpu.VMEM((heads, tok, 2 * DH), BF),
            pltpu.VMEM((2, heads, DH, tok), BF),
            pltpu.VMEM((2, heads, half, tok), BF),
            pltpu.VMEM((2, heads, half, half), F32),
            pltpu.VMEM((2, heads, DH, 2 * DH), F32),
            pltpu.VMEM((2, heads, DH, 2 * DH), BF),
            pltpu.VMEM((2, heads, DH, 2 * DH), BF),
            vec, vec, pltpu.VMEM((heads, 2 * DH, half), BF), vec, vec,
            pltpu.VMEM((heads, 1, half), F32),
            pltpu.SemaphoreType.DMA((6,)),
            pltpu.SemaphoreType.DMA((2 * PIECES * n_head,)),
            pltpu.SemaphoreType.DMA((PIECES * n_head,)),
            pltpu.SemaphoreType.DMA((copies,)),
            pltpu.SemaphoreType.DMA((copies,)),
        ],
        compiler_params=pltpu.CompilerParams(
            collective_id=0, has_side_effects=True, vmem_limit_bytes=48 * 1024 * 1024
        ),
    )(*(
        pltpu.with_memory_space_constraint(array, pltpu.HBM)
        for array in (ridge_scale, key_rows, values, d_layer, out_weight, saved_solutions)
    ))
    return pl.pallas_call(
        store,
        name="store",
        out_shape=[flat, flat, flat],
        in_specs=[vmem] * 5,
        out_specs=[hbm, hbm, hbm],
        scratch_shapes=[pltpu.VMEM((heads, tok, DH), F32), pltpu.SemaphoreType.DMA((3, heads))],
        compiler_params=pltpu.CompilerParams(vmem_limit_bytes=8 * 1024 * 1024),
    )(*(pltpu.with_memory_space_constraint(result, pltpu.VMEM) for result in results))


def solution(mesh):
    return jax.shard_map(
        body,
        mesh=mesh,
        in_specs=(
            P("seq", "head"),
            P("seq", "head"),
            P("seq", "head"),
            P("head", None),
            P("seq", "head"),
            P("head"),
        ),
        out_specs=(P("seq", "head"), P("seq", "head"), P("seq", "head")),
        check_vma=False,
    )
```
